256 devices in a mesh: batch: 4 (over z_hi), seq: 64 (over y, x, z_lo, core).
Axes of the slice: x: 4, y: 4, z: 8 (z_hi: 4, z_lo: 2; z = z_hi * 2 + z_lo), core: 2. Of those that a mesh axis runs over, the one named last changes fastest.
Arguments:
- tokens: bfloat16 [2, 64, 8192], P(None, 'batch', 'seq'), may hold values from -8 to 8
- norm_gain: bfloat16 [8192], P('seq'), may hold values from 0.5 to 1.5
- w_qkv: bfloat16 [8192, 10240], P('batch', 'seq'), may hold values from -0.0625 to 0.0625
- w_out: bfloat16 [8192, 8192], P('seq'), may hold values from -1.5 to 1.5
- cache_keys: bfloat16 [64, 8192, 1024], P('batch', 'seq'), may hold values from -120 to 120
- cache_values: bfloat16 [64, 8192, 1024], P('batch', 'seq'), may hold values from -6 to 6
- lengths: int32 [64], P('batch'), may hold values from 2048 to 8190
- positions: int32 [64], P('batch'), may hold values from 0 to 32767
Outputs:
- mixed: bfloat16 [2, 64, 8192], P(None, 'batch', 'seq')
The draws below stay inside these ranges and needn't reach their ends.
Inputs may be any that keep to these rules, and one draw needn't show every extreme that they name: `lengths`: filled cache positions of a sequence; its two new tokens take the next two positions.
All inputs are finite; a program needn't handle non-finite values.
Results may differ from the reference program's by a relative error of at most 0.01255.
The reference program's roundings to bfloat16 on the way (of `normed`, `projected`, `rounded` and `attended`) count: a program that leaves them out, or rounds other values in their place, can miss the bound.
Values may be sent and summed in bfloat16 or wider, within the bound.
A program may use at most 128 MiB of HBM per device.

```python
import math
import jax
import jax.numpy as jnp
from jax import lax

D = 8192
H = 64
KVH = 8
HD = 128
CTX_DEV = 128
SEQS = 64
CTX = 8192
KVW = 1024
QKV = 10240
N_SEQ = 64


def draw_tokens(key, part):
    first, second, third = jax.random.split(jax.random.fold_in(key, 11), 3)
    shape = (2, SEQS, D)
    rising = jnp.exp(jnp.linspace(0.0, math.log(3.0), D)).astype(jnp.float32)
    jitter = jax.random.uniform(third, (1, 1, D), jnp.float32, 0.5, 1.5)
    base = jax.random.normal(first, shape, jnp.float32)
    scales = jnp.exp(jax.random.uniform(second, (2, SEQS, 1), jnp.float32, math.log(0.15), math.log(1.5)))
    return jnp.clip(base * scales * rising * jitter * 0.8, -8.0, 8.0).astype(jnp.bfloat16)


def draw_cache_keys(key, part):
    source = jax.random.fold_in(key, 23)
    base = jax.random.normal(source, (SEQS, CTX, KVW), jnp.float32)
    return jnp.clip(base * 2.0, -12.0, 12.0).astype(jnp.bfloat16)


def set_ends(array, key, low, largest):
    dims = array.shape
    index_at = [jax.random.randint(jax.random.fold_in(key, axis), (), 0, dims[axis]) for axis in range(len(dims))]
    array = array.at[tuple(index_at)].set(low)
    longest = dims.index(max(dims))
    index_at[longest] = (index_at[longest] + 1) % dims[longest]
    return array.at[tuple(index_at)].set(largest)


def strengthened(entries, rng, source, target, shards_of, factor):
    def block_of(position):
        return (jnp.arange(entries.shape[position]) // (entries.shape[position] // shards_of)).reshape((-1,) + (1,) * (entries.ndim - 1 - position))

    one_side = jax.random.permutation(rng, shards_of)[block_of(target)]
    far = (block_of(target) + shards_of // 2) % shards_of
    return jnp.where((block_of(source) == one_side) | (block_of(source) == far), factor * entries, entries)


def levels(rng, dims, shards, low, high):
    def one(position, parts):
        steps = jax.random.uniform(jax.random.fold_in(jax.random.fold_in(rng, 6), position), (parts,), jnp.float32, low / len(shards), high / len(shards))
        return jnp.repeat(jnp.exp(steps), dims[position] // parts).reshape((-1,) + (1,) * (len(dims) - position - 1))

    factor_of = one(*shards[0])
    for cut in shards[1:]:
        factor_of = factor_of * one(*cut)
    return factor_of


def centred(key, shape, scale, limit, cuts=(), kind=jnp.bfloat16):
    result = scale * jax.random.normal(key, shape, jnp.float32)
    if cuts:
        result = result * levels(key, shape, cuts, -0.22, 0.18)
    return jnp.clip(result, -limit, limit).astype(kind)


def heavy_noise(own_key, extent, spread, bound, shards, heavy, dtype=jnp.bfloat16):
    result = spread * jax.random.normal(own_key, extent, jnp.float32)
    if shards:
        result = result * levels(own_key, extent, shards, -0.22, 0.18)
    return jnp.clip(strengthened(result, jax.random.fold_in(own_key, 3), *heavy), -bound, bound).astype(dtype)


def setup_inputs(seed: int = 0) -> dict:
    arg_keys = jax.random.split(jax.random.key(seed), 9)
    return {
        "tokens": draw_tokens(jax.random.fold_in(arg_keys[8], 71), 0),
        "norm_gain": jnp.clip(1.0 + 0.1 * jax.random.normal(arg_keys[1], (D,), jnp.float32), 0.5, 1.5).astype(jnp.bfloat16),
        "w_qkv": centred(arg_keys[2], (D, QKV), D ** -0.5, 0.0625, ((0, 4), (1, 64))),
        "w_out": heavy_noise(arg_keys[3], (H * HD, D), HD ** -0.5, 1.5, ((0, 64),), (0, 1, 64, 4.0)),
        "cache_keys": draw_cache_keys(jax.random.fold_in(arg_keys[8], 71), 0),
        "cache_values": centred(arg_keys[5], (SEQS, CTX, KVW), 1.0, 6.0, ((0, 4), (1, 64))),
        "lengths": set_ends(jax.random.randint(arg_keys[6], (SEQS,), CTX // 4, CTX - 1), jax.random.fold_in(arg_keys[6], 1), CTX // 4, (CTX - 1) - 1).astype(jnp.int32),
        "positions": set_ends(jax.random.randint(arg_keys[7], (SEQS,), 0, 4 * CTX), jax.random.fold_in(arg_keys[7], 1), 0, (4 * CTX) - 1).astype(jnp.int32),
    }


rope_base = 500000.0
epsilon = 1e-05
lowest = -1e+30

def rotate(heads, places):
    half = heads.shape[-1] // 2
    freqs = rope_base ** (-(jnp.arange(half).astype(jnp.float32) * 2.0) / heads.shape[-1])
    angles = places[:, None, None] * freqs
    cosine = jnp.cos(angles)
    sine = jnp.sin(angles)
    first = heads[..., :half]
    second = heads[..., half:]
    return jnp.concatenate([first * cosine - second * sine, second * cosine + first * sine], -1)

def normalize(rows, gain):
    widened = rows.astype(jnp.float32)
    totals = lax.optimization_barrier(jnp.sum(widened * widened, -1, keepdims=True))
    return (widened * lax.rsqrt(totals / rows.shape[-1] + epsilon) * gain.astype(jnp.float32)).astype(jnp.bfloat16)

def reference(tokens, norm_gain, w_qkv, w_out, cache_keys, cache_values, lengths, positions):
    seqs = tokens.shape[1]
    width = tokens.shape[2]
    group = H // KVH
    query_width = H * HD
    pair_width = KVH * HD
    flat = tokens.reshape(2 * seqs, width)
    normed = normalize(flat, norm_gain)
    projected = jnp.dot(normed, w_qkv, preferred_element_type=jnp.float32).astype(jnp.bfloat16)
    places = jnp.concatenate([positions, positions + 1]).astype(jnp.float32)
    queries = rotate(projected[:, :query_width].astype(jnp.float32).reshape(2 * seqs, H, HD), places).astype(jnp.bfloat16)
    fresh_keys = rotate(projected[:, query_width:query_width + pair_width].astype(jnp.float32).reshape(2 * seqs, KVH, HD), places).astype(jnp.bfloat16)
    fresh_values = projected[:, query_width + pair_width:].reshape(2 * seqs, KVH, HD)
    queries = jnp.transpose(queries.reshape(2, seqs, H, HD), (1, 0, 2, 3))
    fresh_keys = jnp.transpose(fresh_keys.reshape(2, seqs, KVH, HD), (1, 0, 2, 3))
    fresh_values = jnp.transpose(fresh_values.reshape(2, seqs, KVH, HD), (1, 0, 2, 3))

    def attend(items):
        query_pair, key_pair, value_pair, keys, values, length = items
        block_keys = keys.reshape(N_SEQ, CTX_DEV, KVH, HD).astype(jnp.float32)
        block_values = values.reshape(N_SEQ, CTX_DEV, KVH, HD).astype(jnp.float32)
        grouped = query_pair.astype(jnp.float32).reshape(2, KVH, group, HD)
        scores = jnp.einsum('tkgd,snkd->tkgsn', grouped, block_keys) / math.sqrt(HD)
        extra = jnp.einsum('tkgd,jkd->tkgj', grouped, key_pair.astype(jnp.float32)) / math.sqrt(HD)
        extra = extra[:, :, :, None, :]
        place = jnp.arange(N_SEQ).astype(jnp.int32)[:, None] * CTX_DEV + jnp.arange(CTX_DEV).astype(jnp.int32)[None, :]
        live_cache = (place < length)[None, None, None, :, :]
        pair_index = jnp.arange(2).astype(jnp.int32)
        owner = (length + pair_index)[None, :] // CTX_DEV == jnp.arange(N_SEQ).astype(jnp.int32)[:, None]
        causal = pair_index[None, :] <= pair_index[:, None]
        live_extra = (owner[None, :, :] & causal[:, None, :])[:, None, None, :, :]
        block_peak = jnp.maximum(lax.optimization_barrier(jnp.max(jnp.where(live_cache, scores, lowest), -1)), lax.optimization_barrier(jnp.max(jnp.where(live_extra, extra, lowest), -1)))
        weights = jnp.where(live_cache, jnp.exp(scores - block_peak[..., None]), 0.0)
        extra_weights = jnp.where(live_extra, jnp.exp(extra - block_peak[..., None]), 0.0)
        block_total = lax.optimization_barrier(jnp.sum(weights, -1)) + lax.optimization_barrier(jnp.sum(extra_weights, -1))
        rounded = lax.optimization_barrier(weights.astype(jnp.bfloat16)).astype(jnp.float32)
        extra_rounded = lax.optimization_barrier(extra_weights.astype(jnp.bfloat16)).astype(jnp.float32)
        block_sum = jnp.einsum('tkgsn,snkd->tkgsd', rounded, block_values)
        block_sum = block_sum + jnp.einsum('tkgsj,jkd->tkgsd', extra_rounded, value_pair.astype(jnp.float32))
        peak = lax.optimization_barrier(jnp.max(block_peak, -1, keepdims=True))
        factor = jnp.exp(block_peak - peak)
        summed = lax.optimization_barrier(jnp.sum(factor[..., None] * block_sum, 3))
        total = lax.optimization_barrier(jnp.sum(factor * block_total, 3))
        return (summed / total[..., None]).astype(jnp.bfloat16).reshape(2, H * HD)
    attended = lax.map(attend, (queries, fresh_keys, fresh_values, cache_keys, cache_values, lengths))
    attended = jnp.transpose(attended, (1, 0, 2)).reshape(2 * seqs, H * HD)
    output = jnp.dot(attended, w_out, preferred_element_type=jnp.float32)
    return (flat.astype(jnp.float32) + output).astype(jnp.bfloat16).reshape(2, seqs, width)
```

```python
import functools
import math

import jax
import jax.numpy as jnp
from jax import lax
from jax.experimental import pallas as pl
from jax.experimental.pallas import tpu as pltpu
from jax.sharding import PartitionSpec as P

D = 8192
H = 64
KVH = 8
HD = 128
MESH = pl.DeviceIdType.MESH

rope_base = 500000.0
epsilon = 1e-05
lowest = -1e30


def gray(i):
    return i ^ (i >> 1)


def kernel(
    tok, gain, cosine, sine, lens, wq_hbm, wo_hbm, k_hbm, v_hbm, out,
    wq, wo, kc, vc,
    sq_out, sq_in, x_in, a_out, a_in, xn,
    part, p_in, q_out, g_in, q32,
    o32, o_out, st_out, o_in, st_in, fac, y_out, y_in,
    hbm_sem, s1_send, s1_recv, sq_send, sq_recv, x_send, x_direct, xf_send, x_fwd, a_send, a_recv,
    p_send, p_recv, g_send, g_direct, gf_send, g_fwd,
    o_send, o_recv, st_send, st_recv, y_send, y_recv,
):
    b = lax.axis_index("batch")
    s = lax.axis_index("seq")
    c = s % 2
    zl = (s // 2) % 2
    x = (s // 4) % 4
    y = s // 16
    m = s % 4
    q = s // 4
    j16 = s % 16
    partner = s + 1 - 2 * c

    def remote(src, dst, send, recv, bb, ss):
        return pltpu.make_async_remote_copy(
            src_ref=src, dst_ref=dst, send_sem=send, recv_sem=recv,
            device_id=(bb, ss), device_id_type=MESH,
        )

    def take(sem, ref):
        pltpu.make_async_copy(ref, ref, sem).wait()

    loads = [
        pltpu.make_async_copy(src, dst, hbm_sem.at[i])
        for i, (src, dst) in enumerate(((wq_hbm, wq), (k_hbm, kc), (v_hbm, vc), (wo_hbm, wo)))
    ]
    for load in loads:
        load.start()

    bar = pltpu.get_barrier_semaphore()

    def greet(bb, ss):
        pl.semaphore_signal(bar, inc=1, device_id=(bb, ss), device_id_type=MESH)

    def greet_near(i, _):
        db = 1 + i // 4
        greet((b + db) % 4, ((y + i % 4) % 4) * 16 + j16)
        return 0

    lax.fori_loop(0, 12, greet_near, 0)

    def greet_column(i, _):
        greet((b + 1 + i // 3) % 4, q * 4 + (m + 1 + i % 3) % 4)
        return 0

    lax.fori_loop(0, 9, greet_column, 0)

    def greet_group(i, _):
        greet(b, (s + i) % 64)
        return 0

    lax.fori_loop(1, 64, greet_group, 0)

    widened = tok[...].astype(jnp.float32)
    squares = jnp.concatenate([widened * widened] * 4, axis=0)
    row_group = lax.broadcasted_iota(jnp.int32, (128, 128), 0) // 32
    squares = jnp.where(row_group == b, squares, 0.0)
    sq_out[0:1, :] = jnp.sum(squares.T, axis=0, keepdims=True)
    sq_out[1:2, :] = gain[...].astype(jnp.float32)
    my_rows = pl.ds(pl.multiple_of(b * 32, 32), 32)
    sq_in[y * 4 + b] = sq_out[...]

    @pl.when(b == y)
    def _():
        x_in[j16, my_rows, :] = tok[...]

    q32[pl.ds(80 * 32, 128), :] = jnp.zeros((128, 128), jnp.float32)

    pl.semaphore_wait(bar, 84)

    def send_rows(i, _):
        yy = (y + 3 - i) % 4

        @pl.when((b != y) | (yy != y))
        def _():
            remote(
                tok, x_in.at[j16, my_rows], s1_send, s1_recv.at[b], y, yy * 16 + j16
            ).start()

        return 0

    lax.fori_loop(0, 4, send_rows, 0)

    def send_squares(i, _):
        remote(
            sq_out, sq_in.at[y * 4 + b], sq_send, sq_recv,
            (b + i // 4) % 4, ((y + i % 4) % 4) * 16 + j16,
        ).start()
        return 0

    lax.fori_loop(1, 16, send_squares, 0)

    for i, off in enumerate((0, 1, 3, 2)):
        bb = (b + off) % 4
        piece = x_in.at[j16, pl.ds(pl.multiple_of(bb * 32, 32), 32)]
        if off == 0:
            @pl.when(b != y)
            def _():
                take(s1_recv.at[bb], piece)
        else:
            take(s1_recv.at[bb], piece)

        def send_piece(t, _):
            tt = 7 - t
            xx = (x + gray(tt // 2)) % 4
            zz = (zl + tt) % 2
            cc = jnp.where(tt == 0, 1 - c, c)
            remote(
                piece, piece, x_send, x_direct.at[j16], b, ((y * 4 + xx) * 2 + zz) * 2 + cc
            ).start()
            return 0

        lax.fori_loop(0, 8, send_piece, 0)

    take(sq_recv, sq_in.at[pl.ds(0, 15)])
    a_out[0:1, :] = jnp.sum(sq_in[:, 0:1, :], axis=0)
    a_out[1:2, :] = sq_in[b * 4 + b][1:2, :]
    a_in[j16] = a_out[...]

    def send_stats(i, _):
        remote(
            a_out, a_in.at[j16], a_send, a_recv, b, y * 16 + (j16 + i) % 16
        ).start()
        return 0

    lax.fori_loop(1, 16, send_stats, 0)

    def forward_block(t, _):
        xx = (x + gray(t // 2)) % 4
        zz = (zl + t) % 2
        jj = (xx * 2 + zz) * 2 + c
        block = x_in.at[jj]
        take(x_direct.at[jj], block)
        remote(block, block, xf_send, x_fwd, b, partner).start()
        return 0

    lax.fori_loop(1, 8, forward_block, 0)
    jp = j16 + 1 - 2 * c
    take(x_direct.at[jp], x_in.at[jp])
    take(x_fwd, x_in.at[pl.ds(0, 7)])
    take(a_recv, a_in.at[pl.ds(0, 15)])

    totals = jnp.sum(a_in[:, 0:1, :], axis=0)
    inverse = lax.rsqrt(totals / D + epsilon)
    inverse = jnp.broadcast_to(inverse, (128, 128)).T
    for j in range(16):
        xn[:, j * 128 : (j + 1) * 128] = (
            x_in[j].astype(jnp.float32) * inverse * a_in[j][1:2, :]
        ).astype(jnp.bfloat16)
    loads[0].wait()
    product = jnp.dot(xn[...], wq[...], preferred_element_type=jnp.float32)
    product = jnp.concatenate([product, jnp.zeros((128, 96), jnp.float32)], axis=1)
    product = pltpu.roll(product, 32 * m, 1)
    part[...] = product.reshape(16, 8, 256)
    p_in[b * 4 + m] = part[b * 4 + m]

    def send_part(i, _):
        bb = (b + gray(3 - i // 4)) % 4
        mm = (m + 3 - i % 4) % 4
        remote(
            part.at[bb * 4 + mm], p_in.at[b * 4 + m], p_send, p_recv, bb, q * 4 + mm
        ).start()
        return 0

    lax.fori_loop(0, 15, send_part, 0)
    take(p_recv, p_in.at[pl.ds(0, 15)])

    rows8 = pl.ds(pl.multiple_of(m * 8, 8), 8)
    cos8 = cosine[rows8, :]
    sin8 = sine[rows8, :]
    sums = [p_in[mm] + p_in[4 + mm] + p_in[8 + mm] + p_in[12 + mm] for mm in range(4)]
    for j in range(5):
        head = None
        if j < 4:
            head = sums[j][:, :128]
        if j > 0:
            upper = sums[j - 1][:, 128:]
            head = upper if head is None else head + upper
        head = head.astype(jnp.bfloat16).astype(jnp.float32)
        turned = head * cos8 + pltpu.roll(head, 64, 1) * sin8
        q_out[j] = jnp.where(q * 5 + j < H + KVH, turned, head).astype(jnp.bfloat16)
    g_in[s] = q_out[...]

    def chip_at(t):
        yy = (y + gray(t // 8)) % 4
        xx = (x + gray((t // 2) % 4)) % 4
        zz = (zl + t) % 2
        return ((yy * 4 + xx) * 2 + zz) * 2

    def send_heads(t, _):
        tt = 31 - t
        cc = jnp.where(tt == 0, 1 - c, c)
        remote(q_out, g_in.at[s], g_send, g_direct.at[s], b, chip_at(tt) + cc).start()
        return 0

    lax.fori_loop(0, 32, send_heads, 0)

    def forward_heads(t, _):
        ss = chip_at(t) + c
        block = g_in.at[ss]
        take(g_direct.at[ss], block)
        remote(block, block, gf_send, g_fwd, b, partner).start()
        return 0

    lax.fori_loop(1, 32, forward_heads, 0)
    take(g_direct.at[partner], g_in.at[partner])
    take(g_fwd, g_in.at[pl.ds(0, 31)])

    def spread(qq, _):
        for mm in range(4):
            block = g_in[qq * 4 + mm].astype(jnp.float32)
            for j in range(5):
                at = pl.multiple_of((qq * 5 + j) * 32 + mm * 8, 8)
                q32[pl.ds(at, 8), :] = block[j]
        return 0

    lax.fori_loop(0, 16, spread, 0)

    loads[1].wait()
    loads[2].wait()
    scale = 1.0 / math.sqrt(HD)
    lane = lax.broadcasted_iota(jnp.int32, (16, 128), 1)
    step = lax.broadcasted_iota(jnp.int32, (16, 128), 0) // 8
    lane8 = lax.broadcasted_iota(jnp.int32, (8, 128), 1)

    def attend(i, _):
        k = (i + s // 8) % 8
        cols = pl.ds(pl.multiple_of(k * 128, 128), 128)
        queries = []
        for bs in range(16):
            for t in range(2):
                queries.append(q32[pl.ds(k * 256 + t * 16 + bs, 8, stride=32), :])
        queries = jnp.concatenate(queries, axis=0).astype(jnp.bfloat16)
        fresh_at = pl.multiple_of((H + k) * 32, 32)
        fresh_keys = q32[pl.ds(fresh_at, 128), :].astype(jnp.bfloat16)
        fresh_at = pl.multiple_of((H + KVH + k) * 32, 32)
        fresh_values = q32[pl.ds(fresh_at, 128), :].astype(jnp.bfloat16)
        over = (((1,), (1,)), ((), ()))
        extra_all = lax.dot_general(
            queries, fresh_keys, over, preferred_element_type=jnp.float32
        )
        stats = jnp.zeros((8, 128), jnp.float32)
        extra_weights = []
        sums_of = []
        for bs in range(16):
            length = lens[bs]
            rows = slice(bs * 16, bs * 16 + 16)
            scores = (
                lax.dot_general(
                    queries[rows], kc[bs, :, cols], over, preferred_element_type=jnp.float32
                )
                * scale
            )
            live = lane < length - s * 128
            which = lane // 16
            live_extra = (
                (lane % 16 == bs) & (which <= step) & (lane < 32) & ((length + which) // 128 == s)
            )
            scores = jnp.where(live, scores, lowest)
            extra = jnp.where(live_extra, extra_all[rows] * scale, lowest)
            peak = jnp.max(jnp.maximum(scores, extra), axis=1, keepdims=True)
            weights = jnp.where(live, jnp.exp(scores - peak), 0.0)
            weights_extra = jnp.where(live_extra, jnp.exp(extra - peak), 0.0)
            total = jnp.sum(weights + weights_extra, axis=1, keepdims=True)
            extra_weights.append(weights_extra.astype(jnp.bfloat16))
            sums_of.append(
                jnp.dot(
                    weights.astype(jnp.bfloat16), vc[bs, :, cols], preferred_element_type=jnp.float32
                )
            )
            for t in range(2):
                stats = jnp.where(lane8 == t * 16 + bs, total[t * 8 : t * 8 + 8], stats)
                stats = jnp.where(lane8 == 32 + t * 16 + bs, peak[t * 8 : t * 8 + 8], stats)
        extra_sums = jnp.dot(
            jnp.concatenate(extra_weights, axis=0), fresh_values, preferred_element_type=jnp.float32
        )
        for bs in range(16):
            for t in range(2):
                at = bs * 16 + t * 8
                o32[pl.ds(t * 16 + bs, 8, stride=32), :] = (
                    sums_of[bs][t * 8 : t * 8 + 8] + extra_sums[at : at + 8]
                )
        for g in range(8):
            o_out[k * 8 + g] = o32[g * 32 : g * 32 + 32, :].astype(jnp.bfloat16)
            st_out[k * 8 + g] = stats[g : g + 1]

        def send_sums(g, _):
            h = k * 8 + g

            @pl.when(h != s)
            def _():
                remote(o_out.at[h], o_in.at[s], o_send, o_recv, b, h).start()
                remote(st_out.at[h], st_in.at[s], st_send, st_recv, b, h).start()

            return 0

        lax.fori_loop(0, 8, send_sums, 0)
        return 0

    lax.fori_loop(0, 8, attend, 0)
    o_in[s] = o_out[s]
    st_in[s] = st_out[s]
    take(st_recv, st_in.at[pl.ds(0, 63)])

    peak = st_in[0]
    for i in range(1, 64):
        peak = jnp.maximum(peak, st_in[i])
    total = jnp.zeros((1, 128), jnp.float32)
    lane1 = lax.broadcasted_iota(jnp.int32, (1, 128), 1)
    for i in range(64):
        row = st_in[i]
        factor = jnp.where((lane1 >= 32) & (lane1 < 64), jnp.exp(row - peak), 0.0)
        fac[i : i + 1, :] = factor
        total = total + factor * pltpu.roll(row, 32, 1)
    fac[64:65, :] = total
    fac[65:128, :] = jnp.zeros((63, 128), jnp.float32)
    factors = fac[...].T[32:64, :]
    take(o_recv, o_in.at[pl.ds(0, 63)])
    summed = jnp.zeros((32, 128), jnp.float32)
    for i in range(64):
        summed = summed + factors[:, i : i + 1] * o_in[i].astype(jnp.float32)
    attended = (summed / factors[:, 64:65]).astype(jnp.bfloat16)

    loads[3].wait()

    def mix(i, _):
        chunk = (i + q + 10) % 16
        cols = pl.ds(pl.multiple_of(chunk * 512, 512), 512)
        values = jnp.dot(attended, wo[:, cols], preferred_element_type=jnp.float32)
        for u in range(4):
            y_out[chunk * 4 + u] = values[:, u * 128 : (u + 1) * 128].astype(jnp.bfloat16)

        def send_mixed(u, _):
            d = chunk * 4 + u

            @pl.when(d != s)
            def _():
                remote(y_out.at[d], y_in.at[s], y_send, y_recv, b, d).start()

            return 0

        lax.fori_loop(0, 4, send_mixed, 0)
        return 0

    lax.fori_loop(0, 16, mix, 0)
    y_in[s] = y_out[s]
    take(y_recv, y_in.at[pl.ds(0, 63)])
    mixed = tok[...].astype(jnp.float32)
    added = jnp.zeros((32, 128), jnp.float32)
    for i in range(64):
        added = added + y_in[i].astype(jnp.float32)
    out[...] = (mixed + added).astype(jnp.bfloat16)

    @pl.when(b != y)
    def _():
        take(s1_send, x_in.at[0])

    @pl.when(b == y)
    def _():
        take(s1_send, x_in.at[0, pl.ds(0, 96)])

    take(sq_send, sq_in.at[pl.ds(0, 15)])
    take(x_send, x_in.at[pl.ds(0, 8)])
    take(xf_send, x_in.at[pl.ds(0, 7)])
    take(a_send, a_in.at[pl.ds(0, 15)])
    take(p_send, p_in.at[pl.ds(0, 15)])
    take(g_send, g_in.at[pl.ds(0, 32)])
    take(gf_send, g_in.at[pl.ds(0, 31)])
    take(o_send, o_in.at[pl.ds(0, 63)])
    take(st_send, st_in.at[pl.ds(0, 63)])
    take(y_send, y_in.at[pl.ds(0, 63)])


def shards(tokens, norm_gain, w_qkv, w_out, cache_keys, cache_values, lengths, positions):
    seqs = tokens.shape[1]
    local_width = tokens.shape[2]
    rows = 2 * seqs
    places = jnp.concatenate([positions, positions + 1]).astype(jnp.float32)
    half = HD // 2
    freqs = rope_base ** (-(jnp.arange(half).astype(jnp.float32) * 2.0) / HD)
    angles = places[:, None] * freqs
    cosine = jnp.cos(angles)
    sine = jnp.sin(angles)
    cosine = jnp.concatenate([cosine, cosine], axis=1)
    sine = jnp.concatenate([-sine, sine], axis=1)
    f32, bf16 = jnp.float32, jnp.bfloat16
    vmem, dma = pltpu.VMEM, pltpu.SemaphoreType.DMA
    whole = pl.BlockSpec(memory_space=pltpu.VMEM)
    hbm = pl.BlockSpec(memory_space=pl.ANY)
    out = pl.pallas_call(
        kernel,
        out_shape=jax.ShapeDtypeStruct((rows, local_width), bf16),
        in_specs=[whole] * 4 + [pl.BlockSpec(memory_space=pltpu.SMEM)] + [hbm] * 4,
        out_specs=whole,
        scratch_shapes=[
            vmem(w_qkv.shape, bf16),
            vmem(w_out.shape, bf16),
            vmem(cache_keys.shape, bf16),
            vmem(cache_values.shape, bf16),
            vmem((2, 128), f32),
            vmem((16, 2, 128), f32),
            vmem((16, 128, 128), bf16),
            vmem((2, 128), f32),
            vmem((16, 2, 128), f32),
            vmem((128, 2048), bf16),
            vmem((16, 8, 256), f32),
            vmem((16, 8, 256), f32),
            vmem((5, 8, 128), bf16),
            vmem((64, 5, 8, 128), bf16),
            vmem((84 * 32, 128), f32),
            vmem((256, 128), f32),
            vmem((64, 32, 128), bf16),
            vmem((64, 1, 128), f32),
            vmem((64, 32, 128), bf16),
            vmem((64, 1, 128), f32),
            vmem((128, 128), f32),
            vmem((64, 32, 128), bf16),
            vmem((64, 32, 128), bf16),
            dma((4,)),
            dma, dma((4,)), dma, dma, dma, dma((16,)), dma, dma, dma, dma,
            dma, dma, dma, dma((64,)), dma, dma,
            dma, dma, dma, dma, dma, dma,
        ],
        compiler_params=pltpu.CompilerParams(
            collective_id=0, has_side_effects=True, vmem_limit_bytes=60 * 1024 * 1024
        ),
        name="layer",
    )(
        tokens.reshape(rows, local_width), norm_gain.reshape(1, local_width), cosine, sine, lengths,
        w_qkv, w_out, cache_keys, cache_values,
    )
    return out.reshape(2, seqs, local_width)


def solution(mesh):
    return jax.shard_map(
        shards,
        mesh=mesh,
        in_specs=(
            P(None, "batch", "seq"),
            P("seq"),
            P("batch", "seq"),
            P("seq", None),
            P("batch", "seq", None),
            P("batch", "seq", None),
            P("batch"),
            P("batch"),
        ),
        out_specs=P(None, "batch", "seq"),
        check_vma=False,
    )
```

```python
import math

import jax
import jax.numpy as jnp
import numpy as np
from jax import lax
from jax.experimental import pallas as pl
from jax.experimental.pallas import tpu as pltpu
from jax.sharding import PartitionSpec as P

D = 8192
H = 64
KVH = 8
HD = 128
MESH = pl.DeviceIdType.MESH

rope_base = 500000.0
epsilon = 1e-05
lowest = -1e30
floor = -1e29


def gray(i):
    return i ^ (i >> 1)


def kernel(
    tok, gain, freqs, lens, places, wq_hbm, wo_hbm, k_hbm, v_hbm, out,
    wq, wo, kc, vc,
    sq_out, sq_in, x_in, a_out, a_in, xn,
    part, p_in, q_out, g_in, q32,
    dead, dead_extra, raw, raw_extra, wts, wts_extra, peaks, sums, own,
    o32, o_out, st_out, o_in, st_in, fac, att, y_out, y_in,
    hbm_sem, swap_send, swap_recv,
    s1_send, s1_recv, sq_send, sq_recv, x_send, x_direct, xf_send, x_fwd, a_send, a_recv,
    p_send, p_recv, g_send, g_direct, gf_send, g_fwd,
    o_send, o_recv, st_send, st_recv, pair_recv, att_send, att_recv, y_send, y_recv,
):
    b = lax.axis_index("batch")
    s = lax.axis_index("seq")
    c = s % 2
    zl = (s // 2) % 2
    x = (s // 4) % 4
    y = s // 16
    m = s % 4
    q = s // 4
    j16 = s % 16
    partner = s + 1 - 2 * c
    half = s // 32
    chip = s // 2

    def remote(src, dst, send, recv, bb, ss):
        return pltpu.make_async_remote_copy(
            src_ref=src, dst_ref=dst, send_sem=send, recv_sem=recv,
            device_id=(bb, ss), device_id_type=MESH,
        )

    def take(sem, ref):
        pltpu.make_async_copy(ref, ref, sem).wait()

    def halves(cc):
        cols = pl.ds(pl.multiple_of(cc * 512, 512), 512)
        wide = pl.ds(pl.multiple_of(cc * 4096, 4096), 4096)
        return (
            (k_hbm.at[:, :, cols], kc.at[c]),
            (v_hbm.at[:, :, cols], vc.at[c]),
            (wo_hbm.at[:, wide], wo.at[c]),
        )

    loads = [
        pltpu.make_async_copy(src, dst, hbm_sem.at[i])
        for i, (src, dst) in enumerate(((wq_hbm, wq), *halves(c)))
    ]
    swaps = [
        remote(src, dst, swap_send.at[i], swap_recv.at[i], b, partner)
        for i, (src, dst) in enumerate(halves(1 - c))
    ]
    for load in loads:
        load.start()

    bar = pltpu.get_barrier_semaphore()

    def greet(bb, ss):
        pl.semaphore_signal(bar, inc=1, device_id=(bb, ss), device_id_type=MESH)

    def greet_near(i, _):
        db = 1 + i // 4
        greet((b + db) % 4, ((y + i % 4) % 4) * 16 + j16)
        return 0

    lax.fori_loop(0, 12, greet_near, 0)

    def greet_column(i, _):
        greet((b + 1 + i // 3) % 4, q * 4 + (m + 1 + i % 3) % 4)
        return 0

    lax.fori_loop(0, 9, greet_column, 0)

    def greet_group(i, _):
        greet(b, (s + i) % 64)
        return 0

    lax.fori_loop(1, 64, greet_group, 0)

    widened = tok[...].astype(jnp.float32)
    squares = jnp.concatenate([widened * widened] * 4, axis=0)
    row_group = lax.broadcasted_iota(jnp.int32, (128, 128), 0) // 32
    squares = jnp.where(row_group == b, squares, 0.0)
    sq_out[0:1, :] = jnp.sum(squares.T, axis=0, keepdims=True)
    sq_out[1:2, :] = gain[...].astype(jnp.float32)
    my_rows = pl.ds(pl.multiple_of(b * 32, 32), 32)
    sq_in[y * 4 + b] = sq_out[...]

    @pl.when(b == y)
    def _():
        x_in[j16, my_rows, :] = tok[...]

    q32[pl.ds(80 * 32, 128), :] = jnp.zeros((128, 128), jnp.float32)

    row8 = lax.broadcasted_iota(jnp.int32, (8, 128), 0)
    lane8 = lax.broadcasted_iota(jnp.int32, (8, 128), 1)
    place = jnp.zeros((8, 128), jnp.int32)
    for r in range(8):
        place = jnp.where(row8 == r, places[(m % 2) * 8 + r] + m // 2, place)
    angle = place.astype(jnp.float32) * freqs[...]
    cos8 = jnp.cos(angle)
    sin8 = jnp.sin(angle)
    sin8 = jnp.where(lane8 < 64, -sin8, sin8)

    lane = lax.broadcasted_iota(jnp.int32, (16, 128), 1)
    step = lax.broadcasted_iota(jnp.int32, (16, 128), 0) // 8
    which = lane // 16
    for cb in range(2):
        block = s - c + cb
        for bs in range(16):
            rows = pl.ds(cb * 256 + bs * 16, 16)
            dead[rows, :] = jnp.where(lane < lens[bs] - block * 128, 0.0, lowest)
            place = lax.shift_right_arithmetic(lens[bs] + which, 7)
            seen = (lane % 16 == bs) & (which <= step) & (lane < 32) & (place == block)
            dead_extra[rows, :] = jnp.where(seen, 0.0, lowest)

    pl.semaphore_wait(bar, 84)

    def send_rows(i, _):
        yy = (y + 3 - i) % 4

        @pl.when((b != y) | (yy != y))
        def _():
            remote(
                tok, x_in.at[j16, my_rows], s1_send, s1_recv.at[b], y, yy * 16 + j16
            ).start()

        return 0

    lax.fori_loop(0, 4, send_rows, 0)

    def send_squares(i, _):
        remote(
            sq_out, sq_in.at[y * 4 + b], sq_send, sq_recv,
            (b + i // 4) % 4, ((y + i % 4) % 4) * 16 + j16,
        ).start()
        return 0

    lax.fori_loop(1, 16, send_squares, 0)

    swaps[0].start()
    swaps[2].start()

    for i, off in enumerate((0, 1, 3, 2)):
        bb = (b + off) % 4
        piece = x_in.at[j16, pl.ds(pl.multiple_of(bb * 32, 32), 32)]
        if off == 0:
            @pl.when(b != y)
            def _():
                take(s1_recv.at[bb], piece)
        else:
            take(s1_recv.at[bb], piece)

        def send_piece(t, _):
            tt = 7 - t
            xx = (x + gray(tt // 2)) % 4
            zz = (zl + tt) % 2
            cc = jnp.where(tt == 0, 1 - c, c)
            remote(
                piece, piece, x_send, x_direct.at[j16], b, ((y * 4 + xx) * 2 + zz) * 2 + cc
            ).start()
            return 0

        lax.fori_loop(0, 8, send_piece, 0)

    take(sq_recv, sq_in.at[pl.ds(0, 15)])
    a_out[0:1, :] = jnp.sum(sq_in[:, 0:1, :], axis=0)
    a_out[1:2, :] = sq_in[b * 4 + b][1:2, :]
    a_in[j16] = a_out[...]

    def send_stats(i, _):
        remote(
            a_out, a_in.at[j16], a_send, a_recv, b, y * 16 + (j16 + i) % 16
        ).start()
        return 0

    lax.fori_loop(1, 16, send_stats, 0)

    def forward_block(t, _):
        xx = (x + gray(t // 2)) % 4
        zz = (zl + t) % 2
        jj = (xx * 2 + zz) * 2 + c
        block = x_in.at[jj]
        take(x_direct.at[jj], block)
        remote(block, block, xf_send, x_fwd, b, partner).start()
        return 0

    lax.fori_loop(1, 8, forward_block, 0)
    jp = j16 + 1 - 2 * c
    take(x_direct.at[jp], x_in.at[jp])
    take(x_fwd, x_in.at[pl.ds(0, 7)])
    take(a_recv, a_in.at[pl.ds(0, 15)])

    totals = jnp.sum(a_in[:, 0:1, :], axis=0)
    inverse = lax.rsqrt(totals / D + epsilon)
    inverse = jnp.broadcast_to(inverse, (128, 128)).T
    for j in range(16):
        xn[:, j * 128 : (j + 1) * 128] = (
            x_in[j].astype(jnp.float32) * inverse * a_in[j][1:2, :]
        ).astype(jnp.bfloat16)
    loads[0].wait()
    over = (((1,), (1,)), ((), ()))
    product = lax.dot_general(xn[...], wq[...], over, preferred_element_type=jnp.float32)
    product = jnp.concatenate([product, jnp.zeros((128, 96), jnp.float32)], axis=1)
    product = pltpu.roll(product, 32 * m, 1)
    part[...] = product.reshape(16, 8, 256)
    p_in[b * 4 + m] = part[b * 4 + m]

    def send_part(i, _):
        bb = (b + gray(3 - i // 4)) % 4
        mm = (m + 3 - i % 4) % 4
        remote(
            part.at[bb * 4 + mm], p_in.at[b * 4 + m], p_send, p_recv, bb, q * 4 + mm
        ).start()
        return 0

    lax.fori_loop(0, 15, send_part, 0)
    swaps[1].start()
    take(p_recv, p_in.at[pl.ds(0, 15)])

    sums = [p_in[mm] + p_in[4 + mm] + p_in[8 + mm] + p_in[12 + mm] for mm in range(4)]
    for j in range(5):
        head = None
        if j < 4:
            head = sums[j][:, :128]
        if j > 0:
            upper = sums[j - 1][:, 128:]
            head = upper if head is None else head + upper
        head = head.astype(jnp.bfloat16).astype(jnp.float32)
        turned = head * cos8 + pltpu.roll(head, 64, 1) * sin8
        q_out[j] = jnp.where(q * 5 + j < H + KVH, turned, head).astype(jnp.bfloat16)
    g_in[s] = q_out[...]

    def chip_at(t):
        yy = (y + gray(t // 8)) % 4
        xx = (x + gray((t // 2) % 4)) % 4
        zz = (zl + t) % 2
        return ((yy * 4 + xx) * 2 + zz) * 2

    def send_heads(t, _):
        tt = 31 - t
        cc = jnp.where(tt == 0, 1 - c, c)
        remote(q_out, g_in.at[s], g_send, g_direct.at[s], b, chip_at(tt) + cc).start()
        return 0

    lax.fori_loop(0, 32, send_heads, 0)

    def forward_heads(t, _):
        ss = chip_at(t) + c
        block = g_in.at[ss]
        take(g_direct.at[ss], block)
        remote(block, block, gf_send, g_fwd, b, partner).start()
        return 0

    lax.fori_loop(1, 32, forward_heads, 0)
    take(g_direct.at[partner], g_in.at[partner])
    take(g_fwd, g_in.at[pl.ds(0, 31)])

    def spread(qq, _):
        for mm in range(4):
            block = g_in[qq * 4 + mm].astype(jnp.float32)
            for j in range(5):
                at = pl.multiple_of((qq * 5 + j) * 32 + mm * 8, 8)
                q32[pl.ds(at, 8), :] = block[j]
        return 0

    lax.fori_loop(0, 16, spread, 0)

    loads[1].wait()
    loads[2].wait()
    swaps[0].wait_recv()
    swaps[1].wait_recv()
    scale = 1.0 / math.sqrt(HD)

    def kv(i):
        return 4 * c + (s // 8 + i) % 4

    def columns_of(i):
        return pl.ds(pl.multiple_of(((s // 8 + i) % 4) * 128, 128), 128)

    queries = {}

    def fetch(i):
        pieces = []
        for bs in range(16):
            for t in range(2):
                pieces.append(q32[pl.ds(kv(i) * 256 + t * 16 + bs, 8, stride=32), :])
        queries[i] = jnp.concatenate(pieces, axis=0).astype(jnp.bfloat16)
        at = pl.multiple_of((H + kv(i)) * 32, 32)
        raw_extra[i % 2] = lax.dot_general(
            queries[i], q32[pl.ds(at, 128), :].astype(jnp.bfloat16), over,
            preferred_element_type=jnp.float32,
        )

    def score(i, hb, cb):
        for bs in range(hb * 8, hb * 8 + 8):
            raw[i % 2, pl.ds(cb * 256 + bs * 16, 16), :] = lax.dot_general(
                queries[i][bs * 16 : bs * 16 + 16], kc[cb, bs, :, columns_of(i)], over,
                preferred_element_type=jnp.float32,
            )

    def weigh(i, hb, cb):
        rows = pl.ds(cb * 256 + hb * 128, 128)
        scores = raw[i % 2, rows, :] * scale + dead[rows, :]
        extra = raw_extra[i % 2, pl.ds(hb * 128, 128), :] * scale + dead_extra[rows, :]
        peak = jnp.max(jnp.maximum(scores, extra), axis=1, keepdims=True)
        peak = jnp.maximum(peak, floor)
        weights = jnp.exp(scores - peak)
        weights_extra = jnp.exp(extra - peak)
        wts[rows, :] = weights.astype(jnp.bfloat16)
        wts_extra[rows, :] = weights_extra.astype(jnp.bfloat16)
        total = jnp.sum(weights + weights_extra, axis=1, keepdims=True)
        peaks[cb, 0] = jnp.broadcast_to(peak, (128, 128))
        peaks[cb, 1] = jnp.broadcast_to(total, (128, 128))

    def gather_values(i, hb, cb):
        rows = pl.ds(cb * 256 + hb * 128, 128)
        at = pl.multiple_of((H + KVH + kv(i)) * 32, 32)
        sums[cb] = jnp.dot(
            wts_extra[rows, :], q32[pl.ds(at, 128), :].astype(jnp.bfloat16),
            preferred_element_type=jnp.float32,
        )
        for bs in range(8):
            own[cb, pl.ds(bs * 16, 16), :] = jnp.dot(
                wts[pl.ds(cb * 256 + hb * 128 + bs * 16, 16), :],
                vc[cb, hb * 8 + bs, :, columns_of(i)],
                preferred_element_type=jnp.float32,
            )

    stats = {}

    def join(i, hb):
        first, second = peaks[0, 0], peaks[1, 0]
        peak = jnp.maximum(first, second)
        first = jnp.exp(first - peak)
        second = jnp.exp(second - peak)
        total = first * peaks[0, 1] + second * peaks[1, 1]
        summed = first * (own[0] + sums[0]) + second * (own[1] + sums[1])
        if hb == 0:
            stats[i] = jnp.zeros((8, 128), jnp.float32)
        for bs in range(8):
            for t in range(2):
                at = bs * 16 + t * 8
                tb = t * 16 + hb * 8 + bs
                o32[i % 2, pl.ds(tb, 8, stride=32), :] = summed[at : at + 8]
                stats[i] = jnp.where(lane8 == tb, total[at : at + 8], stats[i])
                stats[i] = jnp.where(lane8 == 32 + tb, peak[at : at + 8], stats[i])

    def post(i):
        k = kv(i)
        for g in range(8):
            o_out[k * 8 + g] = o32[i % 2, g * 32 : g * 32 + 32, :].astype(jnp.bfloat16)
            st_out[k * 8 + g] = stats[i][g : g + 1]
        for u in range(8):
            h = k * 8 + (s % 8) ^ u

            def send(recv, st_recv):
                remote(o_out.at[h], o_in.at[chip], o_send, recv, b, h).start()
                remote(st_out.at[h], st_in.at[chip], st_send, st_recv, b, h).start()

            if i == 0 and u < 2:
                @pl.when(half != c)
                def _():
                    send(o_recv, st_recv)

                if u == 1:
                    @pl.when(half == c)
                    def _():
                        send(pair_recv.at[0], pair_recv.at[1])
                else:
                    @pl.when(half == c)
                    def _():
                        o_in[chip] = o_out[h]
                        st_in[chip] = st_out[h]
            else:
                send(o_recv, st_recv)

    groups = [(hb, cb) for hb in range(2) for cb in range(2)]
    fetch(0)
    for hb, cb in groups:
        score(0, hb, cb)
    for i in range(4):
        if i < 3:
            fetch(i + 1)
        for hb, cb in groups:
            if i < 3:
                score(i + 1, hb, cb)
            weigh(i, hb, cb)
            gather_values(i, hb, cb)
            if cb == 1:
                join(i, hb)
        post(i)

    take(st_recv, st_in.at[pl.ds(0, 31)])

    @pl.when(half != c)
    def _():
        take(pair_recv.at[1], st_in.at[0])

    peak = st_in[0]
    for i in range(1, 32):
        peak = jnp.maximum(peak, st_in[i])
    total = jnp.zeros((1, 128), jnp.float32)
    lane1 = lax.broadcasted_iota(jnp.int32, (1, 128), 1)
    for i in range(32):
        row = st_in[i]
        factor = jnp.where((lane1 >= 32) & (lane1 < 64), jnp.exp(row - peak), 0.0)
        fac[i : i + 1, :] = factor
        total = total + factor * pltpu.roll(row, 32, 1)
    fac[32:33, :] = total
    fac[33:128, :] = jnp.zeros((95, 128), jnp.float32)
    factors = fac[...].T[32:64, :]
    take(o_recv, o_in.at[pl.ds(0, 31)])

    @pl.when(half != c)
    def _():
        take(pair_recv.at[0], o_in.at[0])

    summed = jnp.zeros((32, 128), jnp.float32)
    for i in range(32):
        summed = summed + factors[:, i : i + 1] * o_in[i].astype(jnp.float32)
    att[c] = (summed / factors[:, 32:33]).astype(jnp.bfloat16)

    swap = remote(att.at[c], att.at[c], att_send, att_recv, b, partner)
    swap.start()
    loads[3].wait()
    swaps[2].wait_recv()
    swap.wait()
    attended = jnp.concatenate([att[0], att[1]], axis=1)
    for i in range(8):
        chunk = (i + s // 4 + 1) % 8
        cols = pl.ds(pl.multiple_of(chunk * 512, 512), 512)
        weights = jnp.concatenate([wo[0, :, cols], wo[1, :, cols]], axis=0)
        values = jnp.dot(attended, weights, preferred_element_type=jnp.float32)
        for u in range(4):
            y_out[chunk * 4 + u] = values[:, u * 128 : (u + 1) * 128].astype(jnp.bfloat16)
        for u in range(4):
            d = c * 32 + chunk * 4 + m ^ u
            mine = y_out.at[chunk * 4 + m ^ u]

            def send_mixed(recv):
                remote(mine, y_in.at[chip], y_send, recv, b, d).start()

            if i == 7 and u < 2:
                @pl.when(half != c)
                def _():
                    send_mixed(y_recv)

                if u == 1:
                    @pl.when(half == c)
                    def _():
                        send_mixed(pair_recv.at[2])
                else:
                    @pl.when(half == c)
                    def _():
                        y_in[chip] = y_out[chunk * 4 + m]
            else:
                send_mixed(y_recv)

    take(y_recv, y_in.at[pl.ds(0, 31)])

    @pl.when(half != c)
    def _():
        take(pair_recv.at[2], y_in.at[0])

    added = jnp.zeros((32, 128), jnp.float32)
    for i in range(32):
        added = added + y_in[i].astype(jnp.float32)
    out[...] = added

    @pl.when(b != y)
    def _():
        take(s1_send, x_in.at[0])

    @pl.when(b == y)
    def _():
        take(s1_send, x_in.at[0, pl.ds(0, 96)])

    take(sq_send, sq_in.at[pl.ds(0, 15)])
    take(x_send, x_in.at[pl.ds(0, 8)])
    take(xf_send, x_in.at[pl.ds(0, 7)])
    take(a_send, a_in.at[pl.ds(0, 15)])
    take(p_send, p_in.at[pl.ds(0, 15)])
    take(g_send, g_in.at[pl.ds(0, 32)])
    take(gf_send, g_in.at[pl.ds(0, 31)])
    for swap in swaps:
        swap.wait_send()

    @pl.when(half == c)
    def _():
        take(o_send, o_in.at[pl.ds(0, 31)])
        take(st_send, st_in.at[pl.ds(0, 31)])
        take(y_send, y_in.at[pl.ds(0, 31)])

    @pl.when(half != c)
    def _():
        take(o_send, o_in)
        take(st_send, st_in)
        take(y_send, y_in)


def shards(tokens, norm_gain, w_qkv, w_out, cache_keys, cache_values, lengths, positions):
    seqs = tokens.shape[1]
    local_width = tokens.shape[2]
    rows = 2 * seqs
    freqs = rope_base ** (-(np.arange(HD // 2, dtype=np.float64) * 2.0) / HD)
    freqs = np.concatenate([freqs, freqs]).astype(np.float32).reshape(1, HD)
    f32, bf16 = jnp.float32, jnp.bfloat16
    vmem, dma = pltpu.VMEM, pltpu.SemaphoreType.DMA
    whole = pl.BlockSpec(memory_space=pltpu.VMEM)
    hbm = pl.BlockSpec(memory_space=pl.ANY)
    out = pl.pallas_call(
        kernel,
        out_shape=jax.ShapeDtypeStruct((rows, local_width), f32),
        in_specs=[whole] * 3 + [pl.BlockSpec(memory_space=pltpu.SMEM)] * 2 + [hbm] * 4,
        out_specs=whole,
        scratch_shapes=[
            vmem(w_qkv.shape[::-1], bf16),
            vmem((2, 128, 4096), bf16),
            vmem((2, 16, 128, 512), bf16),
            vmem((2, 16, 128, 512), bf16),
            vmem((2, 128), f32),
            vmem((16, 2, 128), f32),
            vmem((16, 128, 128), bf16),
            vmem((2, 128), f32),
            vmem((16, 2, 128), f32),
            vmem((128, 2048), bf16),
            vmem((16, 8, 256), f32),
            vmem((16, 8, 256), f32),
            vmem((5, 8, 128), bf16),
            vmem((64, 5, 8, 128), bf16),
            vmem((84 * 32, 128), f32),
            vmem((512, 128), f32),
            vmem((512, 128), f32),
            vmem((2, 512, 128), f32),
            vmem((2, 256, 128), f32),
            vmem((512, 128), bf16),
            vmem((512, 128), bf16),
            vmem((2, 2, 128, 128), f32),
            vmem((2, 128, 128), f32),
            vmem((2, 128, 128), f32),
            vmem((2, 256, 128), f32),
            vmem((64, 32, 128), bf16),
            vmem((64, 1, 128), f32),
            vmem((32, 32, 128), bf16),
            vmem((32, 1, 128), f32),
            vmem((128, 128), f32),
            vmem((2, 32, 128), bf16),
            vmem((32, 32, 128), bf16),
            vmem((32, 32, 128), bf16),
            dma((4,)), dma((3,)), dma((3,)),
            dma, dma((4,)), dma, dma, dma, dma((16,)), dma, dma, dma, dma,
            dma, dma, dma, dma((64,)), dma, dma,
            dma, dma, dma, dma, dma((3,)), dma, dma, dma, dma,
        ],
        compiler_params=pltpu.CompilerParams(
            collective_id=0, has_side_effects=True, vmem_limit_bytes=60 * 1024 * 1024
        ),
        name="layer",
    )(
        tokens.reshape(rows, local_width), norm_gain.reshape(1, local_width), freqs, lengths, positions,
        w_qkv.T, w_out, cache_keys, cache_values,
    )
    return (tokens.astype(f32) + out.reshape(2, seqs, local_width)).astype(bf16)


def solution(mesh):
    return jax.shard_map(
        shards,
        mesh=mesh,
        in_specs=(
            P(None, "batch", "seq"),
            P("seq"),
            P("batch", "seq"),
            P("seq", None),
            P("batch", "seq", None),
            P("batch", "seq", None),
            P("batch"),
            P("batch"),
        ),
        out_specs=P(None, "batch", "seq"),
        check_vma=False,
    )
```

```python
import math

import jax
import jax.numpy as jnp
import numpy as np
from jax import lax
from jax.experimental import pallas as pl
from jax.experimental.pallas import tpu as pltpu
from jax.sharding import PartitionSpec as P

D = 8192
H = 64
KVH = 8
HD = 128
MESH = pl.DeviceIdType.MESH

rope_base = 500000.0
epsilon = 1e-05
lowest = -1e30
floor = -1e29


def gray(i):
    return i ^ (i >> 1)


def kernel(
    tok, gain, freqs, lens, places, wq_hbm, wo_hbm, k_hbm, v_hbm, out,
    wq, wo, kc, vc,
    sq_out, sq_in, x_in, a_out, a_in, xn,
    part, p_in, q_out, g_in, q32,
    dead, dead_extra, raw, raw_extra, wts, wts_extra, peaks, sums, own,
    o32, o_out, st_out, o_in, st_in, fac, y_out, y_in,
    hbm_sem, swap_send, swap_recv,
    s1_send, s1_recv, sq_send, sq_recv, x_send, x_direct, xf_send, x_fwd, a_send, a_recv,
    p_send, p_recv, g_send, g_recv, o_send, o_recv, st_send, st_recv, y_send, y_recv,
):
    b = lax.axis_index("batch")
    s = lax.axis_index("seq")
    c = s % 2
    zl = (s // 2) % 2
    x = (s // 4) % 4
    y = s // 16
    m = s % 4
    q = s // 4
    j16 = s % 16
    partner = s + 1 - 2 * c
    chip = s // 2

    def remote(src, dst, send, recv, bb, ss):
        return pltpu.make_async_remote_copy(
            src_ref=src, dst_ref=dst, send_sem=send, recv_sem=recv,
            device_id=(bb, ss), device_id_type=MESH,
        )

    def take(sem, ref):
        pltpu.make_async_copy(ref, ref, sem).wait()

    def halves(cc):
        return (
            (k_hbm.at[pl.ds(cc * 8, 8)], kc.at[c]),
            (v_hbm.at[pl.ds(cc * 8, 8)], vc.at[c]),
            (wo_hbm, wo.at[c]),
        )

    loads = [
        pltpu.make_async_copy(src, dst, hbm_sem.at[i])
        for i, (src, dst) in enumerate(((wq_hbm, wq), *halves(c)))
    ]
    swaps = [
        remote(src, dst, swap_send.at[i], swap_recv.at[i], b, partner)
        for i, (src, dst) in enumerate(halves(1 - c))
    ]
    for load in loads:
        load.start()

    bar = pltpu.get_barrier_semaphore()

    def greet(bb, ss):
        pl.semaphore_signal(bar, inc=1, device_id=(bb, ss), device_id_type=MESH)

    def greet_near(i, _):
        db = 1 + i // 4
        greet((b + db) % 4, ((y + i % 4) % 4) * 16 + j16)
        return 0

    lax.fori_loop(0, 12, greet_near, 0)

    def greet_column(i, _):
        greet((b + 1 + i // 3) % 4, q * 4 + (m + 1 + i % 3) % 4)
        return 0

    lax.fori_loop(0, 9, greet_column, 0)

    def greet_group(i, _):
        greet(b, (s + i) % 64)
        return 0

    lax.fori_loop(1, 64, greet_group, 0)

    widened = tok[...].astype(jnp.float32)
    squares = jnp.concatenate([widened * widened] * 4, axis=0)
    row_group = lax.broadcasted_iota(jnp.int32, (128, 128), 0) // 32
    squares = jnp.where(row_group == b, squares, 0.0)
    sq_out[0:1, :] = jnp.sum(squares.T, axis=0, keepdims=True)
    sq_out[1:2, :] = gain[...].astype(jnp.float32)
    my_rows = pl.ds(pl.multiple_of(b * 32, 32), 32)
    sq_in[y * 4 + b] = sq_out[...]

    @pl.when(b == y)
    def _():
        x_in[j16, my_rows, :] = tok[...]

    q32[pl.ds(80 * 16, 128), :] = jnp.zeros((128, 128), jnp.float32)

    row8 = lax.broadcasted_iota(jnp.int32, (8, 128), 0)
    lane8 = lax.broadcasted_iota(jnp.int32, (8, 128), 1)
    place = jnp.zeros((8, 128), jnp.int32)
    for r in range(8):
        place = jnp.where(row8 == r, places[(m % 2) * 8 + r] + m // 2, place)
    angle = place.astype(jnp.float32) * freqs[...]
    cos8 = jnp.cos(angle)
    sin8 = jnp.sin(angle)
    sin8 = jnp.where(lane8 < 64, -sin8, sin8)

    lane = lax.broadcasted_iota(jnp.int32, (16, 128), 1)
    step = lax.broadcasted_iota(jnp.int32, (16, 128), 0) // 8
    which = lane // 8
    for cb in range(2):
        block = s - c + cb
        for bs in range(8):
            length = lens[c * 8 + bs]
            rows = pl.ds(cb * 128 + bs * 16, 16)
            dead[rows, :] = jnp.where(lane < length - block * 128, 0.0, lowest)
            place = lax.shift_right_arithmetic(length + which, 7)
            seen = (lane % 8 == bs) & (which <= step) & (lane < 16) & (place == block)
            dead_extra[rows, :] = jnp.where(seen, 0.0, lowest)

    pl.semaphore_wait(bar, 84)

    def send_rows(i, _):
        yy = (y + 3 - i) % 4

        @pl.when((b != y) | (yy != y))
        def _():
            remote(
                tok, x_in.at[j16, my_rows], s1_send, s1_recv.at[b], y, yy * 16 + j16
            ).start()

        return 0

    lax.fori_loop(0, 4, send_rows, 0)

    def send_squares(i, _):
        remote(
            sq_out, sq_in.at[y * 4 + b], sq_send, sq_recv,
            (b + i // 4) % 4, ((y + i % 4) % 4) * 16 + j16,
        ).start()
        return 0

    lax.fori_loop(1, 16, send_squares, 0)

    swaps[0].start()

    for i, off in enumerate((0, 1, 3, 2)):
        bb = (b + off) % 4
        piece = x_in.at[j16, pl.ds(pl.multiple_of(bb * 32, 32), 32)]
        if off == 0:
            @pl.when(b != y)
            def _():
                take(s1_recv.at[bb], piece)
        else:
            take(s1_recv.at[bb], piece)

        def send_piece(t, _):
            tt = 7 - t
            xx = (x + gray(tt // 2)) % 4
            zz = (zl + tt) % 2
            cc = jnp.where(tt == 0, 1 - c, c)
            remote(
                piece, piece, x_send, x_direct.at[j16], b, ((y * 4 + xx) * 2 + zz) * 2 + cc
            ).start()
            return 0

        lax.fori_loop(0, 8, send_piece, 0)

    take(sq_recv, sq_in.at[pl.ds(0, 15)])
    a_out[0:1, :] = jnp.sum(sq_in[:, 0:1, :], axis=0)
    a_out[1:2, :] = sq_in[b * 4 + b][1:2, :]
    a_in[j16] = a_out[...]

    def send_stats(i, _):
        remote(
            a_out, a_in.at[j16], a_send, a_recv, b, y * 16 + (j16 + i) % 16
        ).start()
        return 0

    lax.fori_loop(1, 16, send_stats, 0)

    def forward_block(t, _):
        xx = (x + gray(t // 2)) % 4
        zz = (zl + t) % 2
        jj = (xx * 2 + zz) * 2 + c
        block = x_in.at[jj]
        take(x_direct.at[jj], block)
        remote(block, block, xf_send, x_fwd, b, partner).start()
        return 0

    lax.fori_loop(1, 8, forward_block, 0)
    jp = j16 + 1 - 2 * c
    take(x_direct.at[jp], x_in.at[jp])
    take(x_fwd, x_in.at[pl.ds(0, 7)])
    take(a_recv, a_in.at[pl.ds(0, 15)])

    totals = jnp.sum(a_in[:, 0:1, :], axis=0)
    inverse = lax.rsqrt(totals / D + epsilon)
    inverse = jnp.broadcast_to(inverse, (128, 128)).T
    for j in range(16):
        xn[:, j * 128 : (j + 1) * 128] = (
            x_in[j].astype(jnp.float32) * inverse * a_in[j][1:2, :]
        ).astype(jnp.bfloat16)
    loads[0].wait()
    over = (((1,), (1,)), ((), ()))
    product = lax.dot_general(xn[...], wq[...], over, preferred_element_type=jnp.float32)
    product = jnp.concatenate([product, jnp.zeros((128, 96), jnp.float32)], axis=1)
    product = pltpu.roll(product, 32 * m, 1)
    part[...] = product.reshape(16, 8, 256)
    p_in[b * 4 + m] = part[b * 4 + m]

    def send_part(i, _):
        bb = (b + gray(3 - i // 4)) % 4
        mm = (m + 3 - i % 4) % 4
        remote(
            part.at[bb * 4 + mm], p_in.at[b * 4 + m], p_send, p_recv, bb, q * 4 + mm
        ).start()
        return 0

    lax.fori_loop(0, 15, send_part, 0)
    swaps[1].start()
    swaps[2].start()
    take(p_recv, p_in.at[pl.ds(0, 15)])

    sums = [p_in[mm] + p_in[4 + mm] + p_in[8 + mm] + p_in[12 + mm] for mm in range(4)]
    for j in range(5):
        head = None
        if j < 4:
            head = sums[j][:, :128]
        if j > 0:
            upper = sums[j - 1][:, 128:]
            head = upper if head is None else head + upper
        head = head.astype(jnp.bfloat16).astype(jnp.float32)
        turned = head * cos8 + pltpu.roll(head, 64, 1) * sin8
        q_out[j] = jnp.where(q * 5 + j < H + KVH, turned, head).astype(jnp.bfloat16)
    g_in[chip] = q_out[...]

    def chip_at(t):
        yy = (y + gray(t // 8)) % 4
        xx = (x + gray((t // 2) % 4)) % 4
        zz = (zl + t) % 2
        return ((yy * 4 + xx) * 2 + zz) * 2

    def send_heads(t, _):
        remote(q_out, g_in.at[chip], g_send, g_recv, b, chip_at(31 - t) + c).start()
        return 0

    lax.fori_loop(0, 31, send_heads, 0)
    take(g_recv, g_in.at[pl.ds(0, 31)])

    def spread(qq, _):
        for t in range(2):
            block = g_in[qq * 2 + t].astype(jnp.float32)
            for j in range(5):
                at = pl.multiple_of((qq * 5 + j) * 16 + t * 8, 8)
                q32[pl.ds(at, 8), :] = block[j]
        return 0

    lax.fori_loop(0, 16, spread, 0)

    loads[1].wait()
    loads[2].wait()
    swaps[0].wait_recv()
    swaps[1].wait_recv()
    scale = 1.0 / math.sqrt(HD)

    def kv(i, kh):
        return (s // 16 + i) % 4 * 2 + kh

    def columns_of(i, kh):
        return pl.ds(pl.multiple_of(kv(i, kh) * 128, 128), 128)

    queries = {}

    def fetch(i):
        for kh in range(2):
            pieces = []
            for bs in range(8):
                for t in range(2):
                    pieces.append(q32[pl.ds(kv(i, kh) * 128 + t * 8 + bs, 8, stride=16), :])
            queries[i, kh] = jnp.concatenate(pieces, axis=0).astype(jnp.bfloat16)
            at = pl.multiple_of((H + kv(i, kh)) * 16, 16)
            raw_extra[i % 2, pl.ds(kh * 128, 128), :] = lax.dot_general(
                queries[i, kh], q32[pl.ds(at, 128), :].astype(jnp.bfloat16), over,
                preferred_element_type=jnp.float32,
            )

    def score(i, kh, cb):
        for bs in range(8):
            raw[i % 2, pl.ds(cb * 256 + kh * 128 + bs * 16, 16), :] = lax.dot_general(
                queries[i, kh][bs * 16 : bs * 16 + 16], kc[cb, bs, :, columns_of(i, kh)], over,
                preferred_element_type=jnp.float32,
            )

    def weigh(i, hb, cb):
        rows = pl.ds(cb * 256 + hb * 128, 128)
        scores = raw[i % 2, rows, :] * scale + dead[pl.ds(cb * 128, 128), :]
        extra = raw_extra[i % 2, pl.ds(hb * 128, 128), :] * scale + dead_extra[pl.ds(cb * 128, 128), :]
        peak = jnp.max(jnp.maximum(scores, extra), axis=1, keepdims=True)
        peak = jnp.maximum(peak, floor)
        weights = jnp.exp(scores - peak)
        weights_extra = jnp.exp(extra - peak)
        wts[rows, :] = weights.astype(jnp.bfloat16)
        wts_extra[rows, :] = weights_extra.astype(jnp.bfloat16)
        total = jnp.sum(weights + weights_extra, axis=1, keepdims=True)
        peaks[cb, 0] = jnp.broadcast_to(peak, (128, 128))
        peaks[cb, 1] = jnp.broadcast_to(total, (128, 128))

    def gather_values(i, hb, cb):
        rows = pl.ds(cb * 256 + hb * 128, 128)
        at = pl.multiple_of((H + KVH + kv(i, hb)) * 16, 16)
        sums[cb] = jnp.dot(
            wts_extra[rows, :], q32[pl.ds(at, 128), :].astype(jnp.bfloat16),
            preferred_element_type=jnp.float32,
        )
        for bs in range(8):
            own[cb, pl.ds(bs * 16, 16), :] = jnp.dot(
                wts[pl.ds(cb * 256 + hb * 128 + bs * 16, 16), :],
                vc[cb, bs, :, columns_of(i, hb)],
                preferred_element_type=jnp.float32,
            )

    stats = {}

    def join(i, hb):
        first, second = peaks[0, 0], peaks[1, 0]
        peak = jnp.maximum(first, second)
        first = jnp.exp(first - peak)
        second = jnp.exp(second - peak)
        total = first * peaks[0, 1] + second * peaks[1, 1]
        summed = first * (own[0] + sums[0]) + second * (own[1] + sums[1])
        stat = jnp.zeros((8, 128), jnp.float32)
        for bs in range(8):
            for t in range(2):
                at = bs * 16 + t * 8
                tb = t * 8 + bs
                o32[hb, pl.ds(tb, 8, stride=16), :] = summed[at : at + 8]
                stat = jnp.where(lane8 == tb, total[at : at + 8], stat)
                stat = jnp.where(lane8 == 32 + tb, peak[at : at + 8], stat)
        stats[i, hb] = (stat, pltpu.roll(stat, 16, 1))

    def post(i, hb):
        for p in range(4):
            dest = kv(i, hb) * 4 + p
            o_out[dest] = o32[hb, p * 32 : p * 32 + 32, :].astype(jnp.bfloat16)
            stat, turned = stats[i, hb]
            st_out[dest] = stat[2 * p : 2 * p + 1] + turned[2 * p + 1 : 2 * p + 2]
        for p in range(4):
            dest = kv(i, hb) * 4 + p

            def send():
                remote(o_out.at[dest], o_in.at[chip], o_send, o_recv, b, dest * 2 + c).start()
                remote(st_out.at[dest], st_in.at[chip], st_send, st_recv, b, dest * 2 + c).start()

            if i == 0:
                pl.when(dest != chip)(send)
            else:
                send()

    groups = [(hb, cb) for hb in range(2) for cb in range(2)]
    fetch(0)
    for hb, cb in groups:
        score(0, hb, cb)
    for i in range(4):
        if i < 3:
            fetch(i + 1)
        for hb, cb in groups:
            if i < 3:
                score(i + 1, hb, cb)
            weigh(i, hb, cb)
            gather_values(i, hb, cb)
            if cb == 1:
                join(i, hb)
                post(i, hb)
    o_in[chip] = o_out[chip]
    st_in[chip] = st_out[chip]
    take(st_recv, st_in.at[pl.ds(0, 31)])

    peak = st_in[0]
    for i in range(1, 32):
        peak = jnp.maximum(peak, st_in[i])
    total = jnp.zeros((1, 128), jnp.float32)
    lane1 = lax.broadcasted_iota(jnp.int32, (1, 128), 1)
    for i in range(32):
        row = st_in[i]
        factor = jnp.where((lane1 >= 32) & (lane1 < 64), jnp.exp(row - peak), 0.0)
        fac[i : i + 1, :] = factor
        total = total + factor * pltpu.roll(row, 32, 1)
    fac[32:33, :] = total
    fac[33:128, :] = jnp.zeros((95, 128), jnp.float32)
    factors = fac[...].T[32:64, :]
    take(o_recv, o_in.at[pl.ds(0, 31)])
    summed = jnp.zeros((32, 128), jnp.float32)
    for i in range(32):
        summed = summed + factors[:, i : i + 1] * o_in[i].astype(jnp.float32)
    attended = summed / factors[:, 32:33]
    attended = jnp.concatenate([attended[:16], attended[16:]], axis=1).astype(jnp.bfloat16)

    loads[3].wait()
    swaps[2].wait_recv()
    for i in range(16):
        chunk = (i + q + 1) % 16
        cols = pl.ds(pl.multiple_of(chunk * 512, 512), 512)
        weights = jnp.concatenate([wo[0, :, cols], wo[1, :, cols]], axis=0)
        values = jnp.dot(attended, weights, preferred_element_type=jnp.float32)
        for u in range(4):
            y_out[chunk * 4 + u] = values[:, u * 128 : (u + 1) * 128].astype(jnp.bfloat16)
        for u in range(4):
            d = chunk * 4 + m ^ u
            if i < 15 or u > 0:
                remote(y_out.at[d], y_in.at[c * 32 + chip], y_send, y_recv, b, d).start()
    y_in[c * 32 + chip] = y_out[s]
    take(y_recv, y_in.at[pl.ds(0, 63)])
    for half in range(2):
        added = jnp.zeros((16, 128), jnp.float32)
        for i in range(32):
            added = added + y_in[half * 32 + i].astype(jnp.float32)
        for t in range(2):
            out[t * 16 + half * 8 : t * 16 + half * 8 + 8, :] = added[t * 8 : t * 8 + 8]

    @pl.when(b != y)
    def _():
        take(s1_send, x_in.at[0])

    @pl.when(b == y)
    def _():
        take(s1_send, x_in.at[0, pl.ds(0, 96)])

    take(sq_send, sq_in.at[pl.ds(0, 15)])
    take(x_send, x_in.at[pl.ds(0, 8)])
    take(xf_send, x_in.at[pl.ds(0, 7)])
    take(a_send, a_in.at[pl.ds(0, 15)])
    take(p_send, p_in.at[pl.ds(0, 15)])
    take(g_send, g_in.at[pl.ds(0, 31)])
    for swap in swaps:
        swap.wait_send()
    take(o_send, o_in.at[pl.ds(0, 31)])
    take(st_send, st_in.at[pl.ds(0, 31)])
    take(y_send, y_in.at[pl.ds(0, 63)])


def shards(tokens, norm_gain, w_qkv, w_out, cache_keys, cache_values, lengths, positions):
    seqs = tokens.shape[1]
    local_width = tokens.shape[2]
    rows = 2 * seqs
    freqs = rope_base ** (-(np.arange(HD // 2, dtype=np.float64) * 2.0) / HD)
    freqs = np.concatenate([freqs, freqs]).astype(np.float32).reshape(1, HD)
    f32, bf16 = jnp.float32, jnp.bfloat16
    vmem, dma = pltpu.VMEM, pltpu.SemaphoreType.DMA
    whole = pl.BlockSpec(memory_space=pltpu.VMEM)
    hbm = pl.BlockSpec(memory_space=pl.ANY)
    out = pl.pallas_call(
        kernel,
        out_shape=jax.ShapeDtypeStruct((rows, local_width), f32),
        in_specs=[whole] * 3 + [pl.BlockSpec(memory_space=pltpu.SMEM)] * 2 + [hbm] * 4,
        out_specs=whole,
        scratch_shapes=[
            vmem(w_qkv.shape[::-1], bf16),
            vmem((2, *w_out.shape), bf16),
            vmem((2, 8, 128, 1024), bf16),
            vmem((2, 8, 128, 1024), bf16),
            vmem((2, 128), f32),
            vmem((16, 2, 128), f32),
            vmem((16, 128, 128), bf16),
            vmem((2, 128), f32),
            vmem((16, 2, 128), f32),
            vmem((128, 2048), bf16),
            vmem((16, 8, 256), f32),
            vmem((16, 8, 256), f32),
            vmem((5, 8, 128), bf16),
            vmem((32, 5, 8, 128), bf16),
            vmem((88 * 16, 128), f32),
            vmem((256, 128), f32),
            vmem((256, 128), f32),
            vmem((2, 512, 128), f32),
            vmem((2, 256, 128), f32),
            vmem((512, 128), bf16),
            vmem((512, 128), bf16),
            vmem((2, 2, 128, 128), f32),
            vmem((2, 128, 128), f32),
            vmem((2, 128, 128), f32),
            vmem((2, 128, 128), f32),
            vmem((32, 32, 128), bf16),
            vmem((32, 1, 128), f32),
            vmem((32, 32, 128), bf16),
            vmem((32, 1, 128), f32),
            vmem((128, 128), f32),
            vmem((64, 16, 128), bf16),
            vmem((64, 16, 128), bf16),
            dma((4,)), dma((3,)), dma((3,)),
            dma, dma((4,)), dma, dma, dma, dma((16,)), dma, dma, dma, dma,
            dma, dma, dma, dma, dma, dma, dma, dma, dma, dma,
        ],
        compiler_params=pltpu.CompilerParams(
            collective_id=0, has_side_effects=True, vmem_limit_bytes=60 * 1024 * 1024
        ),
        name="layer",
    )(
        tokens.reshape(rows, local_width), norm_gain.reshape(1, local_width), freqs, lengths, positions,
        w_qkv.T, w_out, cache_keys, cache_values,
    )
    return (tokens.astype(f32) + out.reshape(2, seqs, local_width)).astype(bf16)


def solution(mesh):
    return jax.shard_map(
        shards,
        mesh=mesh,
        in_specs=(
            P(None, "batch", "seq"),
            P("seq"),
            P("batch", "seq"),
            P("seq", None),
            P("batch", "seq", None),
            P("batch", "seq", None),
            P("batch"),
            P("batch"),
        ),
        out_specs=P(None, "batch", "seq"),
        check_vma=False,
    )
```

```python
import math

import jax
import jax.numpy as jnp
import numpy as np
from jax import lax
from jax.experimental import pallas as pl
from jax.experimental.pallas import tpu as pltpu
from jax.sharding import PartitionSpec as P

D = 8192
H = 64
KVH = 8
HD = 128
MESH = pl.DeviceIdType.MESH

rope_base = 500000.0
epsilon = 1e-05
lowest = -1e30
floor = -1e29


def gray(i):
    return i ^ (i >> 1)


def kernel(
    tok, gain, freqs, lens, places, wq_hbm, wo_hbm, k_hbm, v_hbm, out,
    wq, wo, kc, vc,
    sq_out, sq_in, x_in, a_out, a_in, xn,
    part, p_in, q_out, g_in, q32,
    dead, dead_extra, raw, raw_extra, wts, wts_extra, peaks, sums, own,
    o32, o_out, st_out, o_in, st_in, fac, y_out, y_in,
    hbm_sem, swap_send, swap_recv,
    s1_send, s1_recv, sq_send, sq_recv, x_send, x_direct, xf_send, x_fwd, a_send, a_recv,
    p_send, p_recv, g_send, g_recv, o_send, o_recv, st_send, st_recv, y_send, y_recv,
):
    b = lax.axis_index("batch")
    s = lax.axis_index("seq")
    c = s % 2
    zl = (s // 2) % 2
    x = (s // 4) % 4
    y = s // 16
    m = s % 4
    q = s // 4
    j16 = s % 16
    partner = s + 1 - 2 * c
    chip = s // 2

    def remote(src, dst, send, recv, bb, ss):
        return pltpu.make_async_remote_copy(
            src_ref=src, dst_ref=dst, send_sem=send, recv_sem=recv,
            device_id=(bb, ss), device_id_type=MESH,
        )

    def take(sem, ref):
        pltpu.make_async_copy(ref, ref, sem).wait()

    def halves(cc):
        return (
            (k_hbm.at[pl.ds(cc * 8, 8)], kc.at[c]),
            (v_hbm.at[pl.ds(cc * 8, 8)], vc.at[c]),
            (wo_hbm, wo.at[c]),
        )

    loads = [
        pltpu.make_async_copy(src, dst, hbm_sem.at[i])
        for i, (src, dst) in enumerate(((wq_hbm, wq), *halves(c)))
    ]
    swaps = [
        remote(src, dst, swap_send.at[i], swap_recv.at[i], b, partner)
        for i, (src, dst) in enumerate(halves(1 - c))
    ]
    for load in loads:
        load.start()

    bar = pltpu.get_barrier_semaphore()

    def greet(bb, ss):
        pl.semaphore_signal(bar, inc=1, device_id=(bb, ss), device_id_type=MESH)

    def greet_near(i, _):
        greet((b + i // 4) % 4, ((y + i % 4) % 4) * 16 + j16)
        greet(b, y * 16 + (j16 + i) % 16)
        return 0

    lax.fori_loop(1, 16, greet_near, 0)

    widened = tok[...].astype(jnp.float32)
    squares = jnp.concatenate([widened * widened] * 4, axis=0)
    row_group = lax.broadcasted_iota(jnp.int32, (128, 128), 0) // 32
    squares = jnp.where(row_group == b, squares, 0.0)
    sq_out[0:1, :] = jnp.sum(squares.T, axis=0, keepdims=True)
    sq_out[1:2, :] = gain[...].astype(jnp.float32)
    my_rows = pl.ds(pl.multiple_of(b * 32, 32), 32)
    sq_in[y * 4 + b] = sq_out[...]

    @pl.when(b == y)
    def _():
        x_in[j16, my_rows, :] = tok[...]

    q32[pl.ds(80 * 16, 128), :] = jnp.zeros((128, 128), jnp.float32)

    row8 = lax.broadcasted_iota(jnp.int32, (8, 128), 0)
    lane8 = lax.broadcasted_iota(jnp.int32, (8, 128), 1)
    place = jnp.zeros((8, 128), jnp.int32)
    for r in range(8):
        place = jnp.where(row8 == r, places[(m % 2) * 8 + r] + m // 2, place)
    angle = place.astype(jnp.float32) * freqs[...]
    cos8 = jnp.cos(angle)
    sin8 = jnp.sin(angle)
    sin8 = jnp.where(lane8 < 64, -sin8, sin8)

    lane = lax.broadcasted_iota(jnp.int32, (16, 128), 1)
    step = lax.broadcasted_iota(jnp.int32, (16, 128), 0) // 8
    which = lane // 8
    for cb in range(2):
        block = s - c + cb
        for bs in range(8):
            length = lens[c * 8 + bs]
            rows = pl.ds(cb * 128 + bs * 16, 16)
            dead[rows, :] = jnp.where(lane < length - block * 128, 0.0, lowest)
            place = lax.shift_right_arithmetic(length + which, 7)
            seen = (lane % 8 == bs) & (which <= step) & (lane < 16) & (place == block)
            dead_extra[rows, :] = jnp.where(seen, 0.0, lowest)

    pl.semaphore_wait(bar, 30)

    def send_rows(i, _):
        yy = (y + 3 - i) % 4

        @pl.when((b != y) | (yy != y))
        def _():
            remote(
                tok, x_in.at[j16, my_rows], s1_send, s1_recv.at[b], y, yy * 16 + j16
            ).start()

        return 0

    lax.fori_loop(0, 4, send_rows, 0)

    def send_squares(i, _):
        remote(
            sq_out, sq_in.at[y * 4 + b], sq_send, sq_recv,
            (b + i // 4) % 4, ((y + i % 4) % 4) * 16 + j16,
        ).start()
        return 0

    lax.fori_loop(1, 16, send_squares, 0)

    swaps[0].start()

    for i, off in enumerate((0, 1, 3, 2)):
        bb = (b + off) % 4
        piece = x_in.at[j16, pl.ds(pl.multiple_of(bb * 32, 32), 32)]
        if off == 0:
            @pl.when(b != y)
            def _():
                take(s1_recv.at[bb], piece)
        else:
            take(s1_recv.at[bb], piece)

        def send_piece(t, _):
            tt = 7 - t
            xx = (x + gray(tt // 2)) % 4
            zz = (zl + tt) % 2
            cc = jnp.where(tt == 0, 1 - c, c)
            remote(
                piece, piece, x_send, x_direct.at[j16], b, ((y * 4 + xx) * 2 + zz) * 2 + cc
            ).start()
            return 0

        lax.fori_loop(0, 8, send_piece, 0)

    take(sq_recv, sq_in.at[pl.ds(0, 15)])
    a_out[0:1, :] = jnp.sum(sq_in[:, 0:1, :], axis=0)
    a_out[1:2, :] = sq_in[b * 4 + b][1:2, :]
    a_in[j16] = a_out[...]

    def send_stats(i, _):
        remote(
            a_out, a_in.at[j16], a_send, a_recv, b, y * 16 + (j16 + i) % 16
        ).start()
        return 0

    lax.fori_loop(1, 16, send_stats, 0)

    def forward_block(t, _):
        xx = (x + gray(t // 2)) % 4
        zz = (zl + t) % 2
        jj = (xx * 2 + zz) * 2 + c
        block = x_in.at[jj]
        take(x_direct.at[jj], block)
        remote(block, block, xf_send, x_fwd, b, partner).start()
        return 0

    lax.fori_loop(1, 8, forward_block, 0)
    jp = j16 + 1 - 2 * c
    take(x_direct.at[jp], x_in.at[jp])
    take(x_fwd, x_in.at[pl.ds(0, 7)])
    take(a_recv, a_in.at[pl.ds(0, 15)])

    totals = jnp.sum(a_in[:, 0:1, :], axis=0)
    inverse = lax.rsqrt(totals / D + epsilon)
    inverse = jnp.broadcast_to(inverse, (128, 128)).T
    for j in range(16):
        xn[:, j * 128 : (j + 1) * 128] = (
            x_in[j].astype(jnp.float32) * inverse * a_in[j][1:2, :]
        ).astype(jnp.bfloat16)
    loads[0].wait()
    over = (((1,), (1,)), ((), ()))
    product = lax.dot_general(xn[...], wq[...], over, preferred_element_type=jnp.float32)
    product = jnp.concatenate([product, jnp.zeros((128, 96), jnp.float32)], axis=1)
    product = pltpu.roll(product, 32 * m, 1)
    part[...] = product.reshape(16, 8, 256)
    p_in[b * 4 + m] = part[b * 4 + m]

    def send_part(i, _):
        bb = (b + gray(3 - i // 4)) % 4
        mm = (m + 3 - i % 4) % 4
        remote(
            part.at[bb * 4 + mm], p_in.at[b * 4 + m], p_send, p_recv, bb, q * 4 + mm
        ).start()
        return 0

    lax.fori_loop(0, 15, send_part, 0)
    swaps[1].start()
    swaps[2].start()
    take(p_recv, p_in.at[pl.ds(0, 15)])

    sums = [p_in[mm] + p_in[4 + mm] + p_in[8 + mm] + p_in[12 + mm] for mm in range(4)]
    for j in range(5):
        head = None
        if j < 4:
            head = sums[j][:, :128]
        if j > 0:
            upper = sums[j - 1][:, 128:]
            head = upper if head is None else head + upper
        head = head.astype(jnp.bfloat16).astype(jnp.float32)
        turned = head * cos8 + pltpu.roll(head, 64, 1) * sin8
        q_out[j] = jnp.where(q * 5 + j < H + KVH, turned, head).astype(jnp.bfloat16)
    g_in[chip] = q_out[...]

    def chip_at(t):
        yy = (y + gray(t // 8)) % 4
        xx = (x + gray((t // 2) % 4)) % 4
        zz = (zl + t) % 2
        return ((yy * 4 + xx) * 2 + zz) * 2

    def send_heads(t, _):
        remote(q_out, g_in.at[chip], g_send, g_recv, b, chip_at(31 - t) + c).start()
        return 0

    lax.fori_loop(0, 31, send_heads, 0)
    take(g_recv, g_in.at[pl.ds(0, 31)])

    def spread(qq, _):
        for t in range(2):
            block = g_in[qq * 2 + t].astype(jnp.float32)
            for j in range(5):
                at = pl.multiple_of((qq * 5 + j) * 16 + t * 8, 8)
                q32[pl.ds(at, 8), :] = block[j]
        return 0

    lax.fori_loop(0, 16, spread, 0)

    loads[1].wait()
    loads[2].wait()
    swaps[0].wait_recv()
    swaps[1].wait_recv()
    scale = 1.0 / math.sqrt(HD)

    def kv(i, kh):
        return (y + gray(3 - i)) % 4 * 2 + kh

    def columns_of(i, kh):
        return pl.ds(pl.multiple_of(kv(i, kh) * 128, 128), 128)

    queries = {}

    def fetch(i):
        for kh in range(2):
            pieces = []
            for bs in range(8):
                for t in range(2):
                    pieces.append(q32[pl.ds(kv(i, kh) * 128 + t * 8 + bs, 8, stride=16), :])
            queries[i, kh] = jnp.concatenate(pieces, axis=0).astype(jnp.bfloat16)
            at = pl.multiple_of((H + kv(i, kh)) * 16, 16)
            raw_extra[i % 2, pl.ds(kh * 128, 128), :] = lax.dot_general(
                queries[i, kh], q32[pl.ds(at, 128), :].astype(jnp.bfloat16), over,
                preferred_element_type=jnp.float32,
            )

    def score(i, kh, cb):
        for bs in range(8):
            raw[i % 2, pl.ds(cb * 256 + kh * 128 + bs * 16, 16), :] = lax.dot_general(
                queries[i, kh][bs * 16 : bs * 16 + 16], kc[cb, bs, :, columns_of(i, kh)], over,
                preferred_element_type=jnp.float32,
            )

    def weigh(i, hb, cb):
        rows = pl.ds(cb * 256 + hb * 128, 128)
        scores = raw[i % 2, rows, :] * scale + dead[pl.ds(cb * 128, 128), :]
        extra = raw_extra[i % 2, pl.ds(hb * 128, 128), :] * scale + dead_extra[pl.ds(cb * 128, 128), :]
        peak = jnp.max(jnp.maximum(scores, extra), axis=1, keepdims=True)
        peak = jnp.maximum(peak, floor)
        weights = jnp.exp(scores - peak)
        weights_extra = jnp.exp(extra - peak)
        wts[rows, :] = weights.astype(jnp.bfloat16)
        wts_extra[rows, :] = weights_extra.astype(jnp.bfloat16)
        total = jnp.sum(weights + weights_extra, axis=1, keepdims=True)
        peaks[cb, 0] = jnp.broadcast_to(peak, (128, 128))
        peaks[cb, 1] = jnp.broadcast_to(total, (128, 128))

    def gather_values(i, hb, cb):
        rows = pl.ds(cb * 256 + hb * 128, 128)
        at = pl.multiple_of((H + KVH + kv(i, hb)) * 16, 16)
        sums[cb] = jnp.dot(
            wts_extra[rows, :], q32[pl.ds(at, 128), :].astype(jnp.bfloat16),
            preferred_element_type=jnp.float32,
        )
        for bs in range(8):
            own[cb, pl.ds(bs * 16, 16), :] = jnp.dot(
                wts[pl.ds(cb * 256 + hb * 128 + bs * 16, 16), :],
                vc[cb, bs, :, columns_of(i, hb)],
                preferred_element_type=jnp.float32,
            )

    stats = {}

    def join(i, hb):
        first, second = peaks[0, 0], peaks[1, 0]
        peak = jnp.maximum(first, second)
        first = jnp.exp(first - peak)
        second = jnp.exp(second - peak)
        total = first * peaks[0, 1] + second * peaks[1, 1]
        summed = first * (own[0] + sums[0]) + second * (own[1] + sums[1])
        stat = jnp.zeros((8, 128), jnp.float32)
        for bs in range(8):
            for t in range(2):
                at = bs * 16 + t * 8
                tb = t * 8 + bs
                o32[hb, pl.ds(tb, 8, stride=16), :] = summed[at : at + 8]
                stat = jnp.where(lane8 == tb, total[at : at + 8], stat)
                stat = jnp.where(lane8 == 32 + tb, peak[at : at + 8], stat)
        stats[i, hb] = (stat, pltpu.roll(stat, 16, 1))

    def post(i, hb):
        for p in range(4):
            dest = kv(i, hb) * 4 + p
            o_out[dest] = o32[hb, p * 32 : p * 32 + 32, :].astype(jnp.bfloat16)
            stat, turned = stats[i, hb]
            st_out[dest] = stat[2 * p : 2 * p + 1] + turned[2 * p + 1 : 2 * p + 2]
        for p in range(4):
            dest = kv(i, hb) * 4 + p

            def send():
                remote(o_out.at[dest], o_in.at[chip], o_send, o_recv, b, dest * 2 + c).start()
                remote(st_out.at[dest], st_in.at[chip], st_send, st_recv, b, dest * 2 + c).start()

            if i == 3:
                pl.when(dest != chip)(send)
            else:
                send()

    groups = [(hb, cb) for hb in range(2) for cb in range(2)]
    fetch(0)
    for hb, cb in groups:
        score(0, hb, cb)
    for i in range(4):
        if i < 3:
            fetch(i + 1)
        for hb, cb in groups:
            if i < 3:
                score(i + 1, hb, cb)
            weigh(i, hb, cb)
            gather_values(i, hb, cb)
            if cb == 1:
                join(i, hb)
                post(i, hb)
    o_in[chip] = o_out[chip]
    st_in[chip] = st_out[chip]
    take(st_recv, st_in.at[pl.ds(0, 31)])

    peak = st_in[0]
    for i in range(1, 32):
        peak = jnp.maximum(peak, st_in[i])
    total = jnp.zeros((1, 128), jnp.float32)
    lane1 = lax.broadcasted_iota(jnp.int32, (1, 128), 1)
    for i in range(32):
        row = st_in[i]
        factor = jnp.where((lane1 >= 32) & (lane1 < 64), jnp.exp(row - peak), 0.0)
        fac[i : i + 1, :] = factor
        total = total + factor * pltpu.roll(row, 32, 1)
    fac[32:33, :] = total
    fac[33:128, :] = jnp.zeros((95, 128), jnp.float32)
    factors = fac[...].T[32:64, :]
    take(o_recv, o_in.at[pl.ds(0, 31)])
    summed = jnp.zeros((32, 128), jnp.float32)
    for i in range(32):
        summed = summed + factors[:, i : i + 1] * o_in[i].astype(jnp.float32)
    attended = summed / factors[:, 32:33]
    attended = jnp.concatenate([attended[:16], attended[16:]], axis=1).astype(jnp.bfloat16)

    loads[3].wait()
    swaps[2].wait_recv()

    def chunk_at(i):
        return (y + gray(3 - i // 4)) % 4 * 4 + (x + gray(3 - i % 4)) % 4

    def project(i):
        cols = pl.ds(pl.multiple_of(chunk_at(i) * 512, 512), 512)
        weights = jnp.concatenate([wo[0, :, cols], wo[1, :, cols]], axis=0)
        return jnp.dot(attended, weights, preferred_element_type=jnp.float32)

    ahead = 4
    values = [project(i) for i in range(ahead)]
    for i in range(0, 16, ahead):
        now = values
        values = [project(j) for j in range(i + ahead, min(16, i + 2 * ahead))]
        for j in range(ahead):
            for u in range(4):
                y_out[chunk_at(i + j) * 4 + u] = now[j][:, u * 128 : (u + 1) * 128].astype(jnp.bfloat16)
        for j in range(ahead):
            for u in range(4):
                d = chunk_at(i + j) * 4 + m ^ u
                if i + j < 15 or u > 0:
                    remote(y_out.at[d], y_in.at[c * 32 + chip], y_send, y_recv, b, d).start()
    y_in[c * 32 + chip] = y_out[s]
    take(y_recv, y_in.at[pl.ds(0, 63)])
    for half in range(2):
        added = jnp.zeros((16, 128), jnp.float32)
        for i in range(32):
            added = added + y_in[half * 32 + i].astype(jnp.float32)
        for t in range(2):
            out[t * 16 + half * 8 : t * 16 + half * 8 + 8, :] = added[t * 8 : t * 8 + 8]

    @pl.when(b != y)
    def _():
        take(s1_send, x_in.at[0])

    @pl.when(b == y)
    def _():
        take(s1_send, x_in.at[0, pl.ds(0, 96)])

    take(sq_send, sq_in.at[pl.ds(0, 15)])
    take(x_send, x_in.at[pl.ds(0, 8)])
    take(xf_send, x_in.at[pl.ds(0, 7)])
    take(a_send, a_in.at[pl.ds(0, 15)])
    take(p_send, p_in.at[pl.ds(0, 15)])
    take(g_send, g_in.at[pl.ds(0, 31)])
    for swap in swaps:
        swap.wait_send()
    take(o_send, o_in.at[pl.ds(0, 31)])
    take(st_send, st_in.at[pl.ds(0, 31)])
    take(y_send, y_in.at[pl.ds(0, 63)])


def shards(tokens, norm_gain, w_qkv, w_out, cache_keys, cache_values, lengths, positions):
    seqs = tokens.shape[1]
    local_width = tokens.shape[2]
    rows = 2 * seqs
    freqs = rope_base ** (-(np.arange(HD // 2, dtype=np.float64) * 2.0) / HD)
    freqs = np.concatenate([freqs, freqs]).astype(np.float32).reshape(1, HD)
    f32, bf16 = jnp.float32, jnp.bfloat16
    vmem, dma = pltpu.VMEM, pltpu.SemaphoreType.DMA
    whole = pl.BlockSpec(memory_space=pltpu.VMEM)
    hbm = pl.BlockSpec(memory_space=pl.ANY)
    out = pl.pallas_call(
        kernel,
        out_shape=pltpu.VMEM((rows, local_width), f32),
        in_specs=[whole] * 3 + [pl.BlockSpec(memory_space=pltpu.SMEM)] * 2 + [hbm] * 4,
        out_specs=whole,
        scratch_shapes=[
            vmem(w_qkv.shape[::-1], bf16),
            vmem((2, *w_out.shape), bf16),
            vmem((2, 8, 128, 1024), bf16),
            vmem((2, 8, 128, 1024), bf16),
            vmem((2, 128), f32),
            vmem((16, 2, 128), f32),
            vmem((16, 128, 128), bf16),
            vmem((2, 128), f32),
            vmem((16, 2, 128), f32),
            vmem((128, 2048), bf16),
            vmem((16, 8, 256), f32),
            vmem((16, 8, 256), f32),
            vmem((5, 8, 128), bf16),
            vmem((32, 5, 8, 128), bf16),
            vmem((88 * 16, 128), f32),
            vmem((256, 128), f32),
            vmem((256, 128), f32),
            vmem((2, 512, 128), f32),
            vmem((2, 256, 128), f32),
            vmem((512, 128), bf16),
            vmem((512, 128), bf16),
            vmem((2, 2, 128, 128), f32),
            vmem((2, 128, 128), f32),
            vmem((2, 128, 128), f32),
            vmem((2, 128, 128), f32),
            vmem((32, 32, 128), bf16),
            vmem((32, 1, 128), f32),
            vmem((32, 32, 128), bf16),
            vmem((32, 1, 128), f32),
            vmem((128, 128), f32),
            vmem((64, 16, 128), bf16),
            vmem((64, 16, 128), bf16),
            dma((4,)), dma((3,)), dma((3,)),
            dma, dma((4,)), dma, dma, dma, dma((16,)), dma, dma, dma, dma,
            dma, dma, dma, dma, dma, dma, dma, dma, dma, dma,
        ],
        compiler_params=pltpu.CompilerParams(
            collective_id=0, has_side_effects=True, vmem_limit_bytes=60 * 1024 * 1024
        ),
        name="layer",
    )(
        tokens.reshape(rows, local_width), norm_gain.reshape(1, local_width), freqs, lengths, positions,
        w_qkv.T, w_out, cache_keys, cache_values,
    )
    return (tokens.astype(f32) + out.reshape(2, seqs, local_width)).astype(bf16)


def solution(mesh):
    return jax.shard_map(
        shards,
        mesh=mesh,
        in_specs=(
            P(None, "batch", "seq"),
            P("seq"),
            P("batch", "seq"),
            P("seq", None),
            P("batch", "seq", None),
            P("batch", "seq", None),
            P("batch"),
            P("batch"),
        ),
        out_specs=P(None, "batch", "seq"),
        check_vma=False,
    )
```

```python
import math

import jax
import jax.numpy as jnp
import numpy as np
from jax import lax
from jax.experimental import pallas as pl
from jax.experimental.pallas import tpu as pltpu
from jax.sharding import PartitionSpec as P

D = 8192
H = 64
KVH = 8
HD = 128
MESH = pl.DeviceIdType.MESH

rope_base = 500000.0
epsilon = 1e-05
lowest = -1e30
floor = -1e29


def gray(i):
    return i ^ (i >> 1)


def kernel(
    tok, gain, freqs, lens, places, wq_hbm, wo_hbm, k_hbm, v_hbm, out,
    wq, wo, kc, vc,
    sq_out, sq_in, x_in, a_out, a_in, xn,
    part, p_in, q_out, g_in, q32,
    dead, dead_extra, raw, raw_extra, wts, wts_extra, peaks, sums, own,
    o32, o_out, st_out, o_in, st_in, fac, y_out, y_in,
    hbm_sem, swap_send, swap_recv,
    s1_send, s1_recv, sq_send, sq_recv, x_send, x_direct, xl_send, x_last, xf_send, x_fwd, a_send, a_recv,
    p_send, p_recv, g_send, g_recv, o_send, o_recv, st_send, st_recv, y_send, y_recv,
):
    b = lax.axis_index("batch")
    s = lax.axis_index("seq")
    c = s % 2
    zl = (s // 2) % 2
    x = (s // 4) % 4
    y = s // 16
    m = s % 4
    q = s // 4
    j16 = s % 16
    partner = s + 1 - 2 * c
    chip = s // 2

    def remote(src, dst, send, recv, bb, ss):
        return pltpu.make_async_remote_copy(
            src_ref=src, dst_ref=dst, send_sem=send, recv_sem=recv,
            device_id=(bb, ss), device_id_type=MESH,
        )

    def take(sem, ref):
        pltpu.make_async_copy(ref, ref, sem).wait()

    def halves(cc):
        return (
            (k_hbm.at[pl.ds(cc * 8, 8)], kc.at[c]),
            (v_hbm.at[pl.ds(cc * 8, 8)], vc.at[c]),
            (wo_hbm, wo.at[c]),
        )

    loads = [
        pltpu.make_async_copy(src, dst, hbm_sem.at[i])
        for i, (src, dst) in enumerate(((wq_hbm, wq), *halves(c)))
    ]
    swaps = [
        remote(src, dst, swap_send.at[i], swap_recv.at[i], b, partner)
        for i, (src, dst) in enumerate(halves(1 - c))
    ]
    for load in loads:
        load.start()

    bar = pltpu.get_barrier_semaphore()

    def greet(bb, ss):
        pl.semaphore_signal(bar, inc=1, device_id=(bb, ss), device_id_type=MESH)

    def greet_near(i, _):
        greet((b + i // 4) % 4, ((y + i % 4) % 4) * 16 + j16)
        greet(b, y * 16 + (j16 + i) % 16)
        return 0

    lax.fori_loop(1, 16, greet_near, 0)

    widened = tok[...].astype(jnp.float32)
    squares = jnp.concatenate([widened * widened] * 4, axis=0)
    row_group = lax.broadcasted_iota(jnp.int32, (128, 128), 0) // 32
    squares = jnp.where(row_group == b, squares, 0.0)
    sq_out[0:1, :] = jnp.sum(squares.T, axis=0, keepdims=True)
    sq_out[1:2, :] = gain[...].astype(jnp.float32)
    my_rows = pl.ds(pl.multiple_of(b * 32, 32), 32)
    sq_in[y * 4 + b] = sq_out[...]

    @pl.when(b == y)
    def _():
        x_in[j16, my_rows, :] = tok[...]

    q32[pl.ds(80 * 16, 128), :] = jnp.zeros((128, 128), jnp.float32)

    row8 = lax.broadcasted_iota(jnp.int32, (8, 128), 0)
    lane8 = lax.broadcasted_iota(jnp.int32, (8, 128), 1)
    place = jnp.zeros((8, 128), jnp.int32)
    for r in range(8):
        place = jnp.where(row8 == r, places[(m % 2) * 8 + r] + m // 2, place)
    angle = place.astype(jnp.float32) * freqs[...]
    cos8 = jnp.cos(angle)
    sin8 = jnp.sin(angle)
    sin8 = jnp.where(lane8 < 64, -sin8, sin8)

    lane = lax.broadcasted_iota(jnp.int32, (16, 128), 1)
    step = lax.broadcasted_iota(jnp.int32, (16, 128), 0) // 8
    which = lane // 8
    for cb in range(2):
        block = s - c + cb
        for bs in range(8):
            length = lens[c * 8 + bs]
            rows = pl.ds(cb * 128 + bs * 16, 16)
            dead[rows, :] = jnp.where(lane < length - block * 128, 0.0, lowest)
            place = lax.shift_right_arithmetic(length + which, 7)
            seen = (lane % 8 == bs) & (which <= step) & (lane < 16) & (place == block)
            dead_extra[rows, :] = jnp.where(seen, 0.0, lowest)

    pl.semaphore_wait(bar, 30)

    def send_rows(i, _):
        yy = (y + 3 - i) % 4

        @pl.when((b != y) | (yy != y))
        def _():
            remote(
                tok, x_in.at[j16, my_rows], s1_send, s1_recv.at[b], y, yy * 16 + j16
            ).start()

        return 0

    lax.fori_loop(0, 4, send_rows, 0)

    def send_squares(i, _):
        remote(
            sq_out, sq_in.at[y * 4 + b], sq_send, sq_recv,
            (b + i // 4) % 4, ((y + i % 4) % 4) * 16 + j16,
        ).start()
        return 0

    lax.fori_loop(1, 16, send_squares, 0)

    swaps[0].start()

    for i, off in enumerate((0, 1, 3, 2)):
        bb = (b + off) % 4
        piece = x_in.at[j16, pl.ds(pl.multiple_of(bb * 32, 32), 32)]
        if off == 0:
            @pl.when(b != y)
            def _():
                take(s1_recv.at[bb], piece)
        else:
            take(s1_recv.at[bb], piece)

        def send_piece(t, _):
            tt = 7 - t
            xx = (x + gray(tt // 2)) % 4
            zz = (zl + tt) % 2
            cc = jnp.where(tt == 0, 1 - c, c)
            remote(
                piece, piece, x_send, x_direct.at[j16], b, ((y * 4 + xx) * 2 + zz) * 2 + cc
            ).start()
            return 0

        def send_last(t, _):
            tt = 15 - t
            xx = (x + gray(tt // 4)) % 4
            zz = (zl + tt // 2) % 2
            cc = (c + tt) % 2
            remote(
                piece, piece, xl_send, x_last, b, ((y * 4 + xx) * 2 + zz) * 2 + cc
            ).start()
            return 0

        if off == 2:
            lax.fori_loop(0, 15, send_last, 0)
        else:
            lax.fori_loop(0, 8, send_piece, 0)
        if off == 3:
            take(sq_recv, sq_in.at[pl.ds(0, 15)])
            a_out[0:1, :] = jnp.sum(sq_in[:, 0:1, :], axis=0)
            a_out[1:2, :] = sq_in[b * 4 + b][1:2, :]
            a_in[j16] = a_out[...]

            def send_stats(i, _):
                remote(
                    a_out, a_in.at[j16], a_send, a_recv, b, y * 16 + (j16 + i) % 16
                ).start()
                return 0

            lax.fori_loop(1, 16, send_stats, 0)

    early = o_out.at[pl.ds(0, 3)]

    def forward_block(t, _):
        xx = (x + gray(t // 2)) % 4
        zz = (zl + t) % 2
        jj = (xx * 2 + zz) * 2 + c
        take(x_direct.at[jj], early)
        for off in (0, 1, 3):
            bb = (b + off) % 4
            piece = x_in.at[jj, pl.ds(pl.multiple_of(bb * 32, 32), 32)]
            remote(piece, piece, xf_send, x_fwd, b, partner).start()
        return 0

    lax.fori_loop(1, 8, forward_block, 0)
    take(x_direct.at[j16 + 1 - 2 * c], early)
    take(x_fwd, o_out.at[pl.ds(0, 21)])
    take(x_last, o_out.at[pl.ds(0, 15)])
    take(a_recv, a_in.at[pl.ds(0, 15)])

    totals = jnp.sum(a_in[:, 0:1, :], axis=0)
    inverse = lax.rsqrt(totals / D + epsilon)
    inverse = jnp.broadcast_to(inverse, (128, 128)).T
    for j in range(16):
        xn[:, j * 128 : (j + 1) * 128] = (
            x_in[j].astype(jnp.float32) * inverse * a_in[j][1:2, :]
        ).astype(jnp.bfloat16)
    loads[0].wait()
    over = (((1,), (1,)), ((), ()))
    product = lax.dot_general(xn[...], wq[...], over, preferred_element_type=jnp.float32)
    product = jnp.concatenate([product, jnp.zeros((128, 96), jnp.float32)], axis=1)
    product = pltpu.roll(product, 32 * m, 1)
    part[...] = product.reshape(16, 8, 256)
    p_in[b * 4 + m] = part[b * 4 + m]

    def send_part(i, _):
        bb = (b + gray(3 - i // 4)) % 4
        mm = (m + 3 - i % 4) % 4
        remote(
            part.at[bb * 4 + mm], p_in.at[b * 4 + m], p_send, p_recv, bb, q * 4 + mm
        ).start()
        return 0

    lax.fori_loop(0, 15, send_part, 0)
    swaps[1].start()
    swaps[2].start()
    take(p_recv, p_in.at[pl.ds(0, 15)])

    sums = [p_in[mm] + p_in[4 + mm] + p_in[8 + mm] + p_in[12 + mm] for mm in range(4)]
    for j in range(5):
        head = None
        if j < 4:
            head = sums[j][:, :128]
        if j > 0:
            upper = sums[j - 1][:, 128:]
            head = upper if head is None else head + upper
        head = head.astype(jnp.bfloat16).astype(jnp.float32)
        turned = head * cos8 + pltpu.roll(head, 64, 1) * sin8
        q_out[j] = jnp.where(q * 5 + j < H + KVH, turned, head).astype(jnp.bfloat16)
    g_in[chip] = q_out[...]

    def chip_at(t):
        yy = (y + gray(t // 8)) % 4
        xx = (x + gray((t // 2) % 4)) % 4
        zz = (zl + t) % 2
        return ((yy * 4 + xx) * 2 + zz) * 2

    def send_heads(t, _):
        remote(q_out, g_in.at[chip], g_send, g_recv, b, chip_at(31 - t) + c).start()
        return 0

    lax.fori_loop(0, 31, send_heads, 0)
    take(g_recv, g_in.at[pl.ds(0, 31)])

    def spread(qq, _):
        for t in range(2):
            block = g_in[qq * 2 + t].astype(jnp.float32)
            for j in range(5):
                at = pl.multiple_of((qq * 5 + j) * 16 + t * 8, 8)
                q32[pl.ds(at, 8), :] = block[j]
        return 0

    lax.fori_loop(0, 16, spread, 0)

    loads[1].wait()
    loads[2].wait()
    swaps[0].wait_recv()
    swaps[1].wait_recv()
    scale = 1.0 / math.sqrt(HD)

    def kv(i, kh):
        return (y + gray(3 - i)) % 4 * 2 + (x // 2 + 1 + kh) % 2

    def columns_of(i, kh):
        return pl.ds(pl.multiple_of(kv(i, kh) * 128, 128), 128)

    queries = {}

    def fetch(i):
        for kh in range(2):
            pieces = []
            for bs in range(8):
                for t in range(2):
                    pieces.append(q32[pl.ds(kv(i, kh) * 128 + t * 8 + bs, 8, stride=16), :])
            queries[i, kh] = jnp.concatenate(pieces, axis=0).astype(jnp.bfloat16)
            at = pl.multiple_of((H + kv(i, kh)) * 16, 16)
            raw_extra[i % 2, pl.ds(kh * 128, 128), :] = lax.dot_general(
                queries[i, kh], q32[pl.ds(at, 128), :].astype(jnp.bfloat16), over,
                preferred_element_type=jnp.float32,
            )

    def score(i, kh, cb):
        for bs in range(8):
            raw[i % 2, pl.ds(cb * 256 + kh * 128 + bs * 16, 16), :] = lax.dot_general(
                queries[i, kh][bs * 16 : bs * 16 + 16], kc[cb, bs, :, columns_of(i, kh)], over,
                preferred_element_type=jnp.float32,
            )

    def weigh(i, hb, cb):
        rows = pl.ds(cb * 256 + hb * 128, 128)
        scores = raw[i % 2, rows, :] * scale + dead[pl.ds(cb * 128, 128), :]
        extra = raw_extra[i % 2, pl.ds(hb * 128, 128), :] * scale + dead_extra[pl.ds(cb * 128, 128), :]
        peak = jnp.max(jnp.maximum(scores, extra), axis=1, keepdims=True)
        peak = jnp.maximum(peak, floor)
        weights = jnp.exp(scores - peak)
        weights_extra = jnp.exp(extra - peak)
        wts[rows, :] = weights.astype(jnp.bfloat16)
        wts_extra[rows, :] = weights_extra.astype(jnp.bfloat16)
        total = jnp.sum(weights + weights_extra, axis=1, keepdims=True)
        peaks[cb, 0] = jnp.broadcast_to(peak, (128, 128))
        peaks[cb, 1] = jnp.broadcast_to(total, (128, 128))

    def gather_values(i, hb, cb):
        rows = pl.ds(cb * 256 + hb * 128, 128)
        at = pl.multiple_of((H + KVH + kv(i, hb)) * 16, 16)
        sums[cb] = jnp.dot(
            wts_extra[rows, :], q32[pl.ds(at, 128), :].astype(jnp.bfloat16),
            preferred_element_type=jnp.float32,
        )
        for bs in range(8):
            own[cb, pl.ds(bs * 16, 16), :] = jnp.dot(
                wts[pl.ds(cb * 256 + hb * 128 + bs * 16, 16), :],
                vc[cb, bs, :, columns_of(i, hb)],
                preferred_element_type=jnp.float32,
            )

    stats = {}

    def join(i, hb):
        first, second = peaks[0, 0], peaks[1, 0]
        peak = jnp.maximum(first, second)
        first = jnp.exp(first - peak)
        second = jnp.exp(second - peak)
        total = first * peaks[0, 1] + second * peaks[1, 1]
        summed = first * (own[0] + sums[0]) + second * (own[1] + sums[1])
        stat = jnp.zeros((8, 128), jnp.float32)
        for bs in range(8):
            for t in range(2):
                at = bs * 16 + t * 8
                tb = t * 8 + bs
                o32[hb, pl.ds(tb, 8, stride=16), :] = summed[at : at + 8]
                stat = jnp.where(lane8 == tb, total[at : at + 8], stat)
                stat = jnp.where(lane8 == 32 + tb, peak[at : at + 8], stat)
        stats[i, hb] = (stat, pltpu.roll(stat, 16, 1))

    def post(i, hb):
        for p in range(4):
            dest = kv(i, hb) * 4 + p
            o_out[dest] = o32[hb, p * 32 : p * 32 + 32, :].astype(jnp.bfloat16)
            stat, turned = stats[i, hb]
            st_out[dest] = stat[2 * p : 2 * p + 1] + turned[2 * p + 1 : 2 * p + 2]
        for p in range(4):
            dest = kv(i, hb) * 4 + p

            def send():
                remote(o_out.at[dest], o_in.at[chip], o_send, o_recv, b, dest * 2 + c).start()
                remote(st_out.at[dest], st_in.at[chip], st_send, st_recv, b, dest * 2 + c).start()

            if i == 3:
                pl.when(dest != chip)(send)
            else:
                send()

    groups = [(hb, cb) for hb in range(2) for cb in range(2)]
    fetch(0)
    for hb, cb in groups:
        score(0, hb, cb)
    for i in range(4):
        if i < 3:
            fetch(i + 1)
        for hb, cb in groups:
            if i < 3:
                score(i + 1, hb, cb)
            weigh(i, hb, cb)
            gather_values(i, hb, cb)
            if cb == 1:
                join(i, hb)
        for hb in range(2):
            post(i, hb)
    o_in[chip] = o_out[chip]
    st_in[chip] = st_out[chip]
    take(st_recv, st_in.at[pl.ds(0, 31)])

    peak = st_in[0]
    for i in range(1, 32):
        peak = jnp.maximum(peak, st_in[i])
    total = jnp.zeros((1, 128), jnp.float32)
    lane1 = lax.broadcasted_iota(jnp.int32, (1, 128), 1)
    for i in range(32):
        row = st_in[i]
        factor = jnp.where((lane1 >= 32) & (lane1 < 64), jnp.exp(row - peak), 0.0)
        fac[i : i + 1, :] = factor
        total = total + factor * pltpu.roll(row, 32, 1)
    fac[32:33, :] = total
    fac[33:128, :] = jnp.zeros((95, 128), jnp.float32)
    factors = fac[...].T[32:64, :]
    take(o_recv, o_in.at[pl.ds(0, 31)])
    summed = jnp.zeros((32, 128), jnp.float32)
    for i in range(32):
        summed = summed + factors[:, i : i + 1] * o_in[i].astype(jnp.float32)
    attended = summed / factors[:, 32:33]
    attended = jnp.concatenate([attended[:16], attended[16:]], axis=1).astype(jnp.bfloat16)

    loads[3].wait()
    swaps[2].wait_recv()

    def chunk_at(i):
        return (y + gray(3 - i // 4)) % 4 * 4 + (x + gray(3 - i % 4)) % 4

    def project(i):
        cols = pl.ds(pl.multiple_of(chunk_at(i) * 512, 512), 512)
        weights = jnp.concatenate([wo[0, :, cols], wo[1, :, cols]], axis=0)
        return jnp.dot(attended, weights, preferred_element_type=jnp.float32)

    ahead = 4
    values = [project(i) for i in range(ahead)]
    for i in range(0, 16, ahead):
        now = values
        values = [project(j) for j in range(i + ahead, min(16, i + 2 * ahead))]
        for j in range(ahead):
            for u in range(4):
                y_out[chunk_at(i + j) * 4 + u] = now[j][:, u * 128 : (u + 1) * 128].astype(jnp.bfloat16)
        for j in range(ahead):
            for u in range(4):
                d = chunk_at(i + j) * 4 + m ^ u
                if i + j < 15 or u > 0:
                    remote(y_out.at[d], y_in.at[c * 32 + chip], y_send, y_recv, b, d).start()
    y_in[c * 32 + chip] = y_out[s]
    take(y_recv, y_in.at[pl.ds(0, 63)])
    for half in range(2):
        added = jnp.zeros((16, 128), jnp.float32)
        for i in range(32):
            added = added + y_in[half * 32 + i].astype(jnp.float32)
        for t in range(2):
            out[t * 16 + half * 8 : t * 16 + half * 8 + 8, :] = added[t * 8 : t * 8 + 8]

    @pl.when(b != y)
    def _():
        take(s1_send, x_in.at[0])

    @pl.when(b == y)
    def _():
        take(s1_send, x_in.at[0, pl.ds(0, 96)])

    take(sq_send, sq_in.at[pl.ds(0, 15)])
    take(x_send, o_out.at[pl.ds(0, 24)])
    take(xl_send, o_out.at[pl.ds(0, 15)])
    take(xf_send, o_out.at[pl.ds(0, 21)])
    take(a_send, a_in.at[pl.ds(0, 15)])
    take(p_send, p_in.at[pl.ds(0, 15)])
    take(g_send, g_in.at[pl.ds(0, 31)])
    for swap in swaps:
        swap.wait_send()
    take(o_send, o_in.at[pl.ds(0, 31)])
    take(st_send, st_in.at[pl.ds(0, 31)])
    take(y_send, y_in.at[pl.ds(0, 63)])


def shards(tokens, norm_gain, w_qkv, w_out, cache_keys, cache_values, lengths, positions):
    seqs = tokens.shape[1]
    local_width = tokens.shape[2]
    rows = 2 * seqs
    freqs = rope_base ** (-(np.arange(HD // 2, dtype=np.float64) * 2.0) / HD)
    freqs = np.concatenate([freqs, freqs]).astype(np.float32).reshape(1, HD)
    f32, bf16 = jnp.float32, jnp.bfloat16
    vmem, dma = pltpu.VMEM, pltpu.SemaphoreType.DMA
    whole = pl.BlockSpec(memory_space=pltpu.VMEM)
    hbm = pl.BlockSpec(memory_space=pl.ANY)
    out = pl.pallas_call(
        kernel,
        out_shape=pltpu.VMEM((rows, local_width), f32),
        in_specs=[whole] * 3 + [pl.BlockSpec(memory_space=pltpu.SMEM)] * 2 + [hbm] * 4,
        out_specs=whole,
        scratch_shapes=[
            vmem(w_qkv.shape[::-1], bf16),
            vmem((2, *w_out.shape), bf16),
            vmem((2, 8, 128, 1024), bf16),
            vmem((2, 8, 128, 1024), bf16),
            vmem((2, 128), f32),
            vmem((16, 2, 128), f32),
            vmem((16, 128, 128), bf16),
            vmem((2, 128), f32),
            vmem((16, 2, 128), f32),
            vmem((128, 2048), bf16),
            vmem((16, 8, 256), f32),
            vmem((16, 8, 256), f32),
            vmem((5, 8, 128), bf16),
            vmem((32, 5, 8, 128), bf16),
            vmem((88 * 16, 128), f32),
            vmem((256, 128), f32),
            vmem((256, 128), f32),
            vmem((2, 512, 128), f32),
            vmem((2, 256, 128), f32),
            vmem((512, 128), bf16),
            vmem((512, 128), bf16),
            vmem((2, 2, 128, 128), f32),
            vmem((2, 128, 128), f32),
            vmem((2, 128, 128), f32),
            vmem((2, 128, 128), f32),
            vmem((32, 32, 128), bf16),
            vmem((32, 1, 128), f32),
            vmem((32, 32, 128), bf16),
            vmem((32, 1, 128), f32),
            vmem((128, 128), f32),
            vmem((64, 16, 128), bf16),
            vmem((64, 16, 128), bf16),
            dma((4,)), dma((3,)), dma((3,)),
            dma, dma((4,)), dma, dma, dma, dma((16,)), dma, dma, dma, dma, dma, dma,
            dma, dma, dma, dma, dma, dma, dma, dma, dma, dma,
        ],
        compiler_params=pltpu.CompilerParams(
            collective_id=0, has_side_effects=True, vmem_limit_bytes=60 * 1024 * 1024
        ),
        name="layer",
    )(
        tokens.reshape(rows, local_width), norm_gain.reshape(1, local_width), freqs, lengths, positions,
        w_qkv.T, w_out, cache_keys, cache_values,
    )
    return (tokens.astype(f32) + out.reshape(2, seqs, local_width)).astype(bf16)


def solution(mesh):
    return jax.shard_map(
        shards,
        mesh=mesh,
        in_specs=(
            P(None, "batch", "seq"),
            P("seq"),
            P("batch", "seq"),
            P("seq", None),
            P("batch", "seq", None),
            P("batch", "seq", None),
            P("batch"),
            P("batch"),
        ),
        out_specs=P(None, "batch", "seq"),
        check_vma=False,
    )
```

```python
import math

import jax
import jax.numpy as jnp
import numpy as np
from jax import lax
from jax.experimental import pallas as pl
from jax.experimental.pallas import tpu as pltpu
from jax.sharding import PartitionSpec as P

D = 8192
H = 64
KVH = 8
HD = 128
MESH = pl.DeviceIdType.MESH

rope_base = 500000.0
epsilon = 1e-05
lowest = -1e30
floor = -1e29


def gray(i):
    return i ^ (i >> 1)


def kernel(
    tok, gain, freqs, lens, places, wq_hbm, wo_hbm, k_hbm, v_hbm, out,
    wq, wo, kc, vc,
    sq_out, sq_in, x_in, a_out, a_in, xn,
    part, p_in, q_out, g_in, q32,
    dead, dead_extra, raw, raw_extra, wts, wts_extra, peaks, sums, own,
    o32, o_out, st_out, o_in, st_in, fac, y_out, y_in,
    hbm_sem, swap_send, swap_recv,
    s1_send, s1_recv, sq_send, sq_recv, x_send, x_direct, xl_send, x_last, xf_send, x_fwd, a_send, a_recv,
    p_send, p_recv, g_send, g_recv, o_send, o_recv, st_send, st_recv, y_send, y_recv,
):
    b = lax.axis_index("batch")
    s = lax.axis_index("seq")
    c = s % 2
    zl = (s // 2) % 2
    x = (s // 4) % 4
    y = s // 16
    m = s % 4
    q = s // 4
    j16 = s % 16
    partner = s + 1 - 2 * c
    chip = s // 2

    def remote(src, dst, send, recv, bb, ss):
        return pltpu.make_async_remote_copy(
            src_ref=src, dst_ref=dst, send_sem=send, recv_sem=recv,
            device_id=(bb, ss), device_id_type=MESH,
        )

    def take(sem, ref):
        pltpu.make_async_copy(ref, ref, sem).wait()

    def halves(cc):
        return (
            (k_hbm.at[pl.ds(cc * 8, 8)], kc.at[c]),
            (v_hbm.at[pl.ds(cc * 8, 8)], vc.at[c]),
            (wo_hbm, wo.at[c]),
        )

    loads = [
        pltpu.make_async_copy(src, dst, hbm_sem.at[i])
        for i, (src, dst) in enumerate(((wq_hbm, wq), *halves(c)))
    ]
    swaps = [
        remote(src, dst, swap_send.at[i], swap_recv.at[i], b, partner)
        for i, (src, dst) in enumerate(halves(1 - c))
    ]
    for load in loads:
        load.start()

    bar = pltpu.get_barrier_semaphore()

    def greet(bb, ss):
        pl.semaphore_signal(bar, inc=1, device_id=(bb, ss), device_id_type=MESH)

    def greet_near(i, _):
        greet((b + i // 4) % 4, ((y + i % 4) % 4) * 16 + j16)
        greet(b, y * 16 + (j16 + i) % 16)
        return 0

    lax.fori_loop(1, 16, greet_near, 0)

    widened = tok[...].astype(jnp.float32)
    squares = jnp.concatenate([widened * widened] * 4, axis=0)
    row_group = lax.broadcasted_iota(jnp.int32, (128, 128), 0) // 32
    squares = jnp.where(row_group == b, squares, 0.0)
    sq_out[0:1, :] = jnp.sum(squares.T, axis=0, keepdims=True)
    sq_out[1:2, :] = gain[...].astype(jnp.float32)
    my_rows = pl.ds(pl.multiple_of(b * 32, 32), 32)
    sq_in[y * 4 + b] = sq_out[...]

    @pl.when(b == y)
    def _():
        x_in[j16, my_rows, :] = tok[...]

    q32[pl.ds(80 * 16, 128), :] = jnp.zeros((128, 128), jnp.float32)

    row8 = lax.broadcasted_iota(jnp.int32, (8, 128), 0)
    lane8 = lax.broadcasted_iota(jnp.int32, (8, 128), 1)
    place = jnp.zeros((8, 128), jnp.int32)
    for r in range(8):
        place = jnp.where(row8 == r, places[(m % 2) * 8 + r] + m // 2, place)
    angle = place.astype(jnp.float32) * freqs[...]
    cos8 = jnp.cos(angle)
    sin8 = jnp.sin(angle)
    sin8 = jnp.where(lane8 < 64, -sin8, sin8)

    lane = lax.broadcasted_iota(jnp.int32, (16, 128), 1)
    step = lax.broadcasted_iota(jnp.int32, (16, 128), 0) // 8
    which = lane // 8
    for cb in range(2):
        block = s - c + cb
        for bs in range(8):
            length = lens[c * 8 + bs]
            rows = pl.ds(cb * 128 + bs * 16, 16)
            dead[rows, :] = jnp.where(lane < length - block * 128, 0.0, lowest)
            place = lax.shift_right_arithmetic(length + which, 7)
            seen = (lane % 8 == bs) & (which <= step) & (lane < 16) & (place == block)
            dead_extra[rows, :] = jnp.where(seen, 0.0, lowest)

    pl.semaphore_wait(bar, 30)

    def send_rows(i, _):
        yy = (y + 3 - i) % 4

        @pl.when((b != y) | (yy != y))
        def _():
            remote(
                tok, x_in.at[j16, my_rows], s1_send, s1_recv.at[b], y, yy * 16 + j16
            ).start()

        return 0

    lax.fori_loop(0, 4, send_rows, 0)

    def send_squares(i, _):
        remote(
            sq_out, sq_in.at[y * 4 + b], sq_send, sq_recv,
            (b + i // 4) % 4, ((y + i % 4) % 4) * 16 + j16,
        ).start()
        return 0

    lax.fori_loop(1, 16, send_squares, 0)

    swaps[0].start()

    for i, off in enumerate((0, 1, 3, 2)):
        bb = (b + off) % 4
        piece = x_in.at[j16, pl.ds(pl.multiple_of(bb * 32, 32), 32)]
        if off == 0:
            @pl.when(b != y)
            def _():
                take(s1_recv.at[bb], piece)
        else:
            take(s1_recv.at[bb], piece)

        def send_piece(t, _):
            tt = 7 - t
            xx = (x + gray(tt // 2)) % 4
            zz = (zl + tt) % 2
            cc = jnp.where(tt == 0, 1 - c, c)
            remote(
                piece, piece, x_send, x_direct.at[j16], b, ((y * 4 + xx) * 2 + zz) * 2 + cc
            ).start()
            return 0

        def send_last(t, _):
            tt = 15 - t
            xx = (x + gray(tt // 4)) % 4
            zz = (zl + tt // 2) % 2
            cc = (c + tt) % 2
            remote(
                piece, piece, xl_send, x_last, b, ((y * 4 + xx) * 2 + zz) * 2 + cc
            ).start()
            return 0

        if off == 2:
            lax.fori_loop(0, 15, send_last, 0)
        else:
            lax.fori_loop(0, 8, send_piece, 0)
        if off == 3:
            take(sq_recv, sq_in.at[pl.ds(0, 15)])
            a_out[0:1, :] = jnp.sum(sq_in[:, 0:1, :], axis=0)
            a_out[1:2, :] = sq_in[b * 4 + b][1:2, :]
            a_in[j16] = a_out[...]

            def send_stats(i, _):
                remote(
                    a_out, a_in.at[j16], a_send, a_recv, b, y * 16 + (j16 + i) % 16
                ).start()
                return 0

            lax.fori_loop(1, 16, send_stats, 0)

    early = o_out.at[pl.ds(0, 3)]

    def forward_block(t, _):
        xx = (x + gray(t // 2)) % 4
        zz = (zl + t) % 2
        jj = (xx * 2 + zz) * 2 + c
        take(x_direct.at[jj], early)
        for off in (0, 1, 3):
            bb = (b + off) % 4
            piece = x_in.at[jj, pl.ds(pl.multiple_of(bb * 32, 32), 32)]
            remote(piece, piece, xf_send, x_fwd, b, partner).start()
        return 0

    lax.fori_loop(1, 8, forward_block, 0)
    take(x_direct.at[j16 + 1 - 2 * c], early)
    take(x_fwd, o_out.at[pl.ds(0, 21)])
    take(x_last, o_out.at[pl.ds(0, 15)])
    take(a_recv, a_in.at[pl.ds(0, 15)])

    totals = jnp.sum(a_in[:, 0:1, :], axis=0)
    inverse = lax.rsqrt(totals / D + epsilon)
    inverse = jnp.broadcast_to(inverse, (128, 128)).T
    for j in range(16):
        xn[:, j * 128 : (j + 1) * 128] = (
            x_in[j].astype(jnp.float32) * inverse * a_in[j][1:2, :]
        ).astype(jnp.bfloat16)
    loads[0].wait()
    over = (((1,), (1,)), ((), ()))
    product = lax.dot_general(xn[...], wq[...], over, preferred_element_type=jnp.float32)
    product = jnp.concatenate([product, jnp.zeros((128, 96), jnp.float32)], axis=1)
    product = pltpu.roll(product, 32 * m, 1)
    part[...] = product.reshape(16, 8, 256)
    p_in[b * 4 + m] = part[b * 4 + m]

    def send_part(i, _):
        bb = (b + gray(3 - i // 4)) % 4
        mm = (m + 3 - i % 4) % 4
        remote(
            part.at[bb * 4 + mm], p_in.at[b * 4 + m], p_send, p_recv, bb, q * 4 + mm
        ).start()
        return 0

    lax.fori_loop(0, 15, send_part, 0)
    swaps[1].start()
    swaps[2].start()
    take(p_recv, p_in.at[pl.ds(0, 15)])

    sums = [p_in[mm] + p_in[4 + mm] + p_in[8 + mm] + p_in[12 + mm] for mm in range(4)]
    for j in range(5):
        head = None
        if j < 4:
            head = sums[j][:, :128]
        if j > 0:
            upper = sums[j - 1][:, 128:]
            head = upper if head is None else head + upper
        head = head.astype(jnp.bfloat16).astype(jnp.float32)
        turned = head * cos8 + pltpu.roll(head, 64, 1) * sin8
        q_out[j] = jnp.where(q * 5 + j < H + KVH, turned, head).astype(jnp.bfloat16)
    g_in[chip] = q_out[...]

    def chip_at(t):
        yy = (y + gray(t // 8)) % 4
        xx = (x + gray((t // 2) % 4)) % 4
        zz = (zl + t) % 2
        return ((yy * 4 + xx) * 2 + zz) * 2

    def send_heads(t, _):
        remote(q_out, g_in.at[chip], g_send, g_recv, b, chip_at(31 - t) + c).start()
        return 0

    lax.fori_loop(0, 31, send_heads, 0)
    take(g_recv, g_in.at[pl.ds(0, 31)])

    def spread(qq, _):
        for t in range(2):
            block = g_in[qq * 2 + t].astype(jnp.float32)
            for j in range(5):
                at = pl.multiple_of((qq * 5 + j) * 16 + t * 8, 8)
                q32[pl.ds(at, 8), :] = block[j]
        return 0

    lax.fori_loop(0, 16, spread, 0)

    loads[1].wait()
    loads[2].wait()
    swaps[0].wait_recv()
    swaps[1].wait_recv()
    scale = 1.0 / math.sqrt(HD)

    def kv(i, kh):
        return (y + gray(3 - i)) % 4 * 2 + (x // 2 + 1 + kh) % 2

    def columns_of(i, kh):
        return pl.ds(pl.multiple_of(kv(i, kh) * 128, 128), 128)

    queries = {}

    def fetch(i):
        for kh in range(2):
            pieces = []
            for bs in range(8):
                for t in range(2):
                    pieces.append(q32[pl.ds(kv(i, kh) * 128 + t * 8 + bs, 8, stride=16), :])
            queries[i, kh] = jnp.concatenate(pieces, axis=0).astype(jnp.bfloat16)
            at = pl.multiple_of((H + kv(i, kh)) * 16, 16)
            raw_extra[i % 2, pl.ds(kh * 128, 128), :] = lax.dot_general(
                queries[i, kh], q32[pl.ds(at, 128), :].astype(jnp.bfloat16), over,
                preferred_element_type=jnp.float32,
            )

    def score(i, kh, cb):
        for bs in range(8):
            raw[i % 2, pl.ds(cb * 256 + kh * 128 + bs * 16, 16), :] = lax.dot_general(
                queries[i, kh][bs * 16 : bs * 16 + 16], kc[cb, bs, :, columns_of(i, kh)], over,
                preferred_element_type=jnp.float32,
            )

    def weigh(i, hb, cb):
        rows = pl.ds(cb * 256 + hb * 128, 128)
        scores = raw[i % 2, rows, :] * scale + dead[pl.ds(cb * 128, 128), :]
        extra = raw_extra[i % 2, pl.ds(hb * 128, 128), :] * scale + dead_extra[pl.ds(cb * 128, 128), :]
        peak = jnp.max(jnp.maximum(scores, extra), axis=1, keepdims=True)
        peak = jnp.maximum(peak, floor)
        weights = jnp.exp(scores - peak)
        weights_extra = jnp.exp(extra - peak)
        wts[rows, :] = weights.astype(jnp.bfloat16)
        wts_extra[rows, :] = weights_extra.astype(jnp.bfloat16)
        total = jnp.sum(weights + weights_extra, axis=1, keepdims=True)
        peaks[cb, 0] = jnp.broadcast_to(peak, (128, 128))
        peaks[cb, 1] = jnp.broadcast_to(total, (128, 128))

    def gather_values(i, hb, cb):
        rows = pl.ds(cb * 256 + hb * 128, 128)
        at = pl.multiple_of((H + KVH + kv(i, hb)) * 16, 16)
        sums[cb] = jnp.dot(
            wts_extra[rows, :], q32[pl.ds(at, 128), :].astype(jnp.bfloat16),
            preferred_element_type=jnp.float32,
        )
        for bs in range(8):
            own[cb, pl.ds(bs * 16, 16), :] = jnp.dot(
                wts[pl.ds(cb * 256 + hb * 128 + bs * 16, 16), :],
                vc[cb, bs, :, columns_of(i, hb)],
                preferred_element_type=jnp.float32,
            )

    stats = {}

    def join(i, hb):
        first, second = peaks[0, 0], peaks[1, 0]
        peak = jnp.maximum(first, second)
        first = jnp.exp(first - peak)
        second = jnp.exp(second - peak)
        total = first * peaks[0, 1] + second * peaks[1, 1]
        summed = first * (own[0] + sums[0]) + second * (own[1] + sums[1])
        stat = jnp.zeros((8, 128), jnp.float32)
        for bs in range(8):
            for t in range(2):
                at = bs * 16 + t * 8
                tb = t * 8 + bs
                o32[2 * (i % 2) + hb, pl.ds(tb, 8, stride=16), :] = summed[at : at + 8]
                stat = jnp.where(lane8 == tb, total[at : at + 8], stat)
                stat = jnp.where(lane8 == 32 + tb, peak[at : at + 8], stat)
        stats[i, hb] = (stat, pltpu.roll(stat, 16, 1))

    def post(i, hb):
        for p in range(4):
            dest = kv(i, hb) * 4 + p
            o_out[dest] = o32[2 * (i % 2) + hb, p * 32 : p * 32 + 32, :].astype(jnp.bfloat16)
            stat, turned = stats[i, hb]
            st_out[dest] = stat[2 * p : 2 * p + 1] + turned[2 * p + 1 : 2 * p + 2]
        for p in range(4):
            dest = kv(i, hb) * 4 + p

            def send():
                remote(o_out.at[dest], o_in.at[chip], o_send, o_recv, b, dest * 2 + c).start()
                remote(st_out.at[dest], st_in.at[chip], st_send, st_recv, b, dest * 2 + c).start()

            if i == 3:
                pl.when(dest != chip)(send)
            else:
                send()

    groups = [(hb, cb) for hb in range(2) for cb in range(2)]
    fetch(0)
    for hb, cb in groups:
        score(0, hb, cb)
    for i in range(4):
        if i < 3:
            fetch(i + 1)
        for hb, cb in groups:
            if i < 3:
                score(i + 1, hb, cb)
            weigh(i, hb, cb)
            gather_values(i, hb, cb)
            if cb == 1:
                join(i, hb)
            if i > 0 and (hb, cb) == (0, 0):
                post(i - 1, 0)
                post(i - 1, 1)
    post(3, 0)
    post(3, 1)
    o_in[chip] = o_out[chip]
    st_in[chip] = st_out[chip]
    take(st_recv, st_in.at[pl.ds(0, 31)])

    peak = st_in[0]
    for i in range(1, 32):
        peak = jnp.maximum(peak, st_in[i])
    total = jnp.zeros((1, 128), jnp.float32)
    lane1 = lax.broadcasted_iota(jnp.int32, (1, 128), 1)
    for i in range(32):
        row = st_in[i]
        factor = jnp.where((lane1 >= 32) & (lane1 < 64), jnp.exp(row - peak), 0.0)
        fac[i : i + 1, :] = factor
        total = total + factor * pltpu.roll(row, 32, 1)
    fac[32:33, :] = total
    fac[33:128, :] = jnp.zeros((95, 128), jnp.float32)
    factors = fac[...].T[32:64, :]
    take(o_recv, o_in.at[pl.ds(0, 31)])
    summed = jnp.zeros((32, 128), jnp.float32)
    for i in range(32):
        summed = summed + factors[:, i : i + 1] * o_in[i].astype(jnp.float32)
    attended = summed / factors[:, 32:33]
    attended = jnp.concatenate([attended[:16], attended[16:]], axis=1).astype(jnp.bfloat16)

    loads[3].wait()
    swaps[2].wait_recv()

    def chunk_at(i):
        return (y + gray(3 - i // 4)) % 4 * 4 + (x + gray(3 - i % 4)) % 4

    def project(i):
        cols = pl.ds(pl.multiple_of(chunk_at(i) * 512, 512), 512)
        weights = jnp.concatenate([wo[0, :, cols], wo[1, :, cols]], axis=0)
        return jnp.dot(attended, weights, preferred_element_type=jnp.float32)

    ahead = 4
    values = [project(i) for i in range(ahead)]
    for i in range(0, 16, ahead):
        now = values
        values = [project(j) for j in range(i + ahead, min(16, i + 2 * ahead))]
        for j in range(ahead):
            for u in range(4):
                y_out[chunk_at(i + j) * 4 + u] = now[j][:, u * 128 : (u + 1) * 128].astype(jnp.bfloat16)
        for j in range(ahead):
            for u in range(4):
                d = chunk_at(i + j) * 4 + m ^ u
                if i + j < 15 or u > 0:
                    remote(y_out.at[d], y_in.at[c * 32 + chip], y_send, y_recv, b, d).start()
    y_in[c * 32 + chip] = y_out[s]
    take(y_recv, y_in.at[pl.ds(0, 63)])
    for half in range(2):
        added = jnp.zeros((16, 128), jnp.float32)
        for i in range(32):
            added = added + y_in[half * 32 + i].astype(jnp.float32)
        for t in range(2):
            out[t * 16 + half * 8 : t * 16 + half * 8 + 8, :] = added[t * 8 : t * 8 + 8]

    @pl.when(b != y)
    def _():
        take(s1_send, x_in.at[0])

    @pl.when(b == y)
    def _():
        take(s1_send, x_in.at[0, pl.ds(0, 96)])

    take(sq_send, sq_in.at[pl.ds(0, 15)])
    take(x_send, o_out.at[pl.ds(0, 24)])
    take(xl_send, o_out.at[pl.ds(0, 15)])
    take(xf_send, o_out.at[pl.ds(0, 21)])
    take(a_send, a_in.at[pl.ds(0, 15)])
    take(p_send, p_in.at[pl.ds(0, 15)])
    take(g_send, g_in.at[pl.ds(0, 31)])
    for swap in swaps:
        swap.wait_send()
    take(o_send, o_in.at[pl.ds(0, 31)])
    take(st_send, st_in.at[pl.ds(0, 31)])
    take(y_send, y_in.at[pl.ds(0, 63)])


def shards(tokens, norm_gain, w_qkv, w_out, cache_keys, cache_values, lengths, positions):
    seqs = tokens.shape[1]
    local_width = tokens.shape[2]
    rows = 2 * seqs
    freqs = rope_base ** (-(np.arange(HD // 2, dtype=np.float64) * 2.0) / HD)
    freqs = np.concatenate([freqs, freqs]).astype(np.float32).reshape(1, HD)
    f32, bf16 = jnp.float32, jnp.bfloat16
    vmem, dma = pltpu.VMEM, pltpu.SemaphoreType.DMA
    whole = pl.BlockSpec(memory_space=pltpu.VMEM)
    hbm = pl.BlockSpec(memory_space=pl.ANY)
    out = pl.pallas_call(
        kernel,
        out_shape=pltpu.VMEM((rows, local_width), f32),
        in_specs=[whole] * 3 + [pl.BlockSpec(memory_space=pltpu.SMEM)] * 2 + [hbm] * 4,
        out_specs=whole,
        scratch_shapes=[
            vmem(w_qkv.shape[::-1], bf16),
            vmem((2, *w_out.shape), bf16),
            vmem((2, 8, 128, 1024), bf16),
            vmem((2, 8, 128, 1024), bf16),
            vmem((2, 128), f32),
            vmem((16, 2, 128), f32),
            vmem((16, 128, 128), bf16),
            vmem((2, 128), f32),
            vmem((16, 2, 128), f32),
            vmem((128, 2048), bf16),
            vmem((16, 8, 256), f32),
            vmem((16, 8, 256), f32),
            vmem((5, 8, 128), bf16),
            vmem((32, 5, 8, 128), bf16),
            vmem((88 * 16, 128), f32),
            vmem((256, 128), f32),
            vmem((256, 128), f32),
            vmem((2, 512, 128), f32),
            vmem((2, 256, 128), f32),
            vmem((512, 128), bf16),
            vmem((512, 128), bf16),
            vmem((2, 2, 128, 128), f32),
            vmem((2, 128, 128), f32),
            vmem((2, 128, 128), f32),
            vmem((4, 128, 128), f32),
            vmem((32, 32, 128), bf16),
            vmem((32, 1, 128), f32),
            vmem((32, 32, 128), bf16),
            vmem((32, 1, 128), f32),
            vmem((128, 128), f32),
            vmem((64, 16, 128), bf16),
            vmem((64, 16, 128), bf16),
            dma((4,)), dma((3,)), dma((3,)),
            dma, dma((4,)), dma, dma, dma, dma((16,)), dma, dma, dma, dma, dma, dma,
            dma, dma, dma, dma, dma, dma, dma, dma, dma, dma,
        ],
        compiler_params=pltpu.CompilerParams(
            collective_id=0, has_side_effects=True, vmem_limit_bytes=60 * 1024 * 1024
        ),
        name="layer",
    )(
        tokens.reshape(rows, local_width), norm_gain.reshape(1, local_width), freqs, lengths, positions,
        w_qkv.T, w_out, cache_keys, cache_values,
    )
    return (tokens.astype(f32) + out.reshape(2, seqs, local_width)).astype(bf16)


def solution(mesh):
    return jax.shard_map(
        shards,
        mesh=mesh,
        in_specs=(
            P(None, "batch", "seq"),
            P("seq"),
            P("batch", "seq"),
            P("seq", None),
            P("batch", "seq", None),
            P("batch", "seq", None),
            P("batch"),
            P("batch"),
        ),
        out_specs=P(None, "batch", "seq"),
        check_vma=False,
    )
```
